512 devices in a mesh: harm: 4 (over z_hi, core), tx: 16 (over y, x), ty: 8 (over z_lo).
Axes of the slice: x: 4, y: 4, z: 16 (z_hi: 2, z_lo: 8; z = z_hi * 8 + z_lo), core: 2. Of those that a mesh axis runs over, the one named last changes fastest.
Arguments:
- wave_spectrum: float32 [2, 512, 64, 1024], P(None, 'harm', 'tx', 'ty'), may hold values from -6 to 6
- lens_window: int32 [64, 1024], P('tx', 'ty'), may hold values 0 or 1
- medium_label: int32 [64, 1024], P('tx', 'ty'), may hold values from 0 to 7
- thermal_excess_prior: float32 [64, 1024], P('tx', 'ty'), may hold values from -6 to 6
- attenuation_by_kind: float32 [8], replicated, may hold values from 0.2 to 2
- blood_drain_by_kind: float32 [8], replicated, may hold values from 0.02 to 0.2
- diffusivity_by_kind: float32 [8], replicated, may hold values from 0.04 to 0.22
Outputs:
- field_out: float32 [2, 512, 64, 1024], P(None, 'harm', 'tx', 'ty')
- thermal_excess_later: float32 [64, 1024], P('tx', 'ty')
The draws below stay inside these ranges and needn't reach their ends.
All inputs are finite; a program needn't handle non-finite values. No bound on the sum of `lens_window` on one device may be relied on, other than what follows from the above.
Results may differ from the reference program's by a relative error of at most 0.000071.
Values sent between devices are 32-bit elements; how exact they have to be, the bound alone decides.
A program may use at most 64 MiB of HBM per device.

```python
import math
import jax
import jax.numpy as jnp
from jax import lax

HARM = 512
CYCLE_READINGS = 2048
NCLASS = 8
CELLS_LEADING = 64
CELLS_TRAILING = 1024


def set_ends(array, rng, smallest, top_value):
    index_at = [jax.random.randint(jax.random.fold_in(rng, axis), (), 0, length) for axis, length in enumerate(array.shape)]
    main_axis = array.shape.index(max(array.shape))
    beside = index_at[:main_axis] + [(index_at[main_axis] + 1) % array.shape[main_axis]] + index_at[main_axis + 1:]
    return array.at[tuple(index_at)].set(smallest).at[tuple(beside)].set(top_value)


def shard_levels(stream_key, extent, pieces, least, high):
    def one(dim, shards_of):
        heights = jax.random.uniform(jax.random.fold_in(jax.random.fold_in(stream_key, 6), dim), (shards_of,), jnp.float32, least / len(pieces), high / len(pieces))
        return jnp.repeat(jnp.exp(heights), extent[dim] // shards_of).reshape((-1,) + (1,) * (len(extent) - dim - 1))

    level = one(*pieces[0])
    for cut in pieces[1:]:
        level = level * one(*cut)
    return level


def normal_values(key, dims, width, limit, pieces=(), kind=jnp.bfloat16):
    drawn = width * jax.random.normal(key, dims, jnp.float32)
    if pieces:
        drawn = drawn * shard_levels(key, dims, pieces, -0.22, 0.18)
    return jnp.clip(drawn, -limit, limit).astype(kind)


def setup_inputs(seed: int = 0) -> dict:
    streams_of = jax.random.split(jax.random.key(seed), 8)
    wave_spectrum = normal_values(streams_of[0], (2, HARM, CELLS_LEADING, CELLS_TRAILING), 1.0, 6.0, ((1, 4), (2, 16), (3, 8)), jnp.float32)
    lens_window = set_ends((jax.random.randint(streams_of[1], (CELLS_LEADING, CELLS_TRAILING), 0, 3) < 2).astype(jnp.int32), jax.random.fold_in(streams_of[1], 1), 0, 1)
    medium_label = set_ends(jax.random.randint(streams_of[2], (CELLS_LEADING, CELLS_TRAILING), 0, NCLASS), jax.random.fold_in(streams_of[2], 1), 0, NCLASS - 1).astype(jnp.int32)
    thermal_excess_prior = normal_values(streams_of[3], (CELLS_LEADING, CELLS_TRAILING), 1.0, 6.0, ((0, 16), (1, 8)), jnp.float32)
    attenuation_by_kind = jnp.clip(jnp.exp(jax.random.uniform(streams_of[4], (NCLASS,), jnp.float32, math.log(0.2), math.log(2.0))), 0.2, 2.0)
    blood_drain_by_kind = jnp.clip(jnp.exp(jax.random.uniform(streams_of[5], (NCLASS,), jnp.float32, math.log(0.02), math.log(0.2))), 0.02, 0.2)
    diffusivity_by_kind = jnp.clip(jnp.exp(jax.random.uniform(streams_of[6], (NCLASS,), jnp.float32, math.log(0.04), math.log(0.22))), 0.04, 0.22)
    return {"wave_spectrum": wave_spectrum, "lens_window": lens_window, "medium_label": medium_label, "thermal_excess_prior": thermal_excess_prior, "attenuation_by_kind": attenuation_by_kind, "blood_drain_by_kind": blood_drain_by_kind, "diffusivity_by_kind": diffusivity_by_kind}


diffraction_gain = 0.3
nonlinear_gain = 0.3

def laplace(padded):
    center = padded[..., 1:-1, 1:-1]
    return padded[..., 2:, 1:-1] + padded[..., :-2, 1:-1] + padded[..., 1:-1, 2:] + padded[..., 1:-1, :-2] - 4.0 * center

def pad_plane(values):
    widths = [(0, 0)] * (values.ndim - 2) + [(1, 1), (1, 1)]
    return jnp.pad(values, widths)

def build_table(overall):
    moment_grid = jnp.arange(CYCLE_READINGS, dtype=jnp.int32)
    overtone_series = jnp.arange(1, overall + 1, dtype=jnp.int32)
    cycle_argument = moment_grid[:, None] * overtone_series[None, :] % CYCLE_READINGS
    angle = 2.0 * math.pi / CYCLE_READINGS * cycle_argument.astype(jnp.float32)
    return jnp.concatenate([jnp.cos(angle), -jnp.sin(angle)], axis=1)

def reference(wave_spectrum, lens_window, medium_label, thermal_excess_prior, attenuation_by_kind, blood_drain_by_kind, diffusivity_by_kind):
    orders = jnp.arange(1, HARM + 1, dtype=jnp.int32).astype(jnp.float32)
    weight = 0.25 + 0.75 * lens_window.astype(jnp.float32)
    source = wave_spectrum * weight
    block_size = 32 if HARM % 32 == 0 else HARM
    groups = HARM // block_size
    blocked = jnp.moveaxis(source.reshape(2, groups, block_size, CELLS_LEADING, CELLS_TRAILING), 1, 0)
    gains = (diffraction_gain / orders).reshape(groups, block_size, 1, 1)

    def diffract(pair):
        anchor, gain_rate = pair
        current = anchor
        for scale_divider in (4.0, 3.0, 2.0, 1.0):
            bending = gain_rate * laplace(pad_plane(current))
            current = anchor + 1.0 / scale_divider * jnp.stack([-bending[1], bending[0]])
        return current
    advanced = lax.map(diffract, (blocked, gains))
    advanced = jnp.moveaxis(advanced, 0, 1).reshape(2, HARM, CELLS_LEADING, CELLS_TRAILING)
    dft_table = build_table(HARM)
    scale_synth = HARM ** (-0.5)
    scale_analysis = 2.0 * math.sqrt(HARM) / CYCLE_READINGS
    rate = nonlinear_gain / HARM * orders[:, None]
    row_major = jnp.moveaxis(advanced, 2, 0)

    def nonlinear(row_block):
        stacked = row_block.reshape(2 * HARM, CELLS_TRAILING)
        pressure = scale_synth * jnp.dot(dft_table, stacked, precision=lax.Precision.HIGHEST)
        spectrum = scale_analysis * lax.dot_general(dft_table, pressure * pressure, (((0,), (0,)), ((), ())), precision=lax.Precision.HIGHEST)
        real_new = stacked[:HARM] - rate * spectrum[HARM:]
        imag_new = stacked[HARM:] + rate * spectrum[:HARM]
        return jnp.stack([real_new, imag_new])
    updated = lax.map(nonlinear, row_major)
    field_out = jnp.moveaxis(updated, 0, 2)
    heat = lax.optimization_barrier(jnp.sum(orders[:, None, None] * (field_out[0] * field_out[0] + field_out[1] * field_out[1]), axis=0))
    codes = jnp.arange(NCLASS, dtype=jnp.int32)
    onehot = (medium_label[None, :, :] == codes[:, None, None]).astype(jnp.float32)
    absorb_map = lax.optimization_barrier(jnp.sum(attenuation_by_kind[:, None, None] * onehot, axis=0))
    conduct_map = lax.optimization_barrier(jnp.sum(diffusivity_by_kind[:, None, None] * onehot, axis=0))
    perfuse_map = lax.optimization_barrier(jnp.sum(blood_drain_by_kind[:, None, None] * onehot, axis=0))
    deposit = absorb_map * heat / (HARM * HARM)
    thermal_excess_later = thermal_excess_prior
    for repeat in range(4):
        thermal_excess_later = thermal_excess_later + conduct_map * laplace(pad_plane(thermal_excess_later)) - perfuse_map * thermal_excess_later + deposit
    return (field_out, thermal_excess_later)
```

```python
import math

import jax
import jax.numpy as jnp
import numpy as np
from jax import lax
from jax.experimental import pallas as pl
from jax.experimental.pallas import tpu as pltpu
from jax.sharding import PartitionSpec as P

CYCLE_READINGS = 2048
HALF = CYCLE_READINGS // 2
HARMONICS = 512
OWN = 128
ROWS = 4
COLS = 128
CHUNKS = 4
WIDTH = COLS // CHUNKS
PAD = 16
F32 = jnp.float32
BF16 = jnp.bfloat16

diffraction_gain = 0.3
nonlinear_gain = 0.3

TX = 16
TY = 8
AROUND = [(dy, dx) for dy in (-1, 0, 1) for dx in (-1, 0, 1) if (dy, dx) != (0, 0)]


def trig(product, period):
    angle = 2.0 * np.pi * (product % period) / period
    return np.cos(angle).astype(np.float32), np.sin(angle).astype(np.float32)


def table_factors():
    n = np.arange(1, HARMONICS + 1, dtype=np.int64)
    fine_c, fine_s = trig(n[:, None] * (2 * np.arange(128)[None, :] + 1), 2 * CYCLE_READINGS)
    coarse_c, coarse_s = trig(np.arange(8)[:, None] * np.arange(1, 17)[None, :], 16)
    coarse_c = np.repeat(coarse_c[:, :, None], 128, axis=2)
    coarse_s = np.repeat(coarse_s[:, :, None], 128, axis=2)
    far_c, far_s = trig(np.arange(64)[:, None] * n[None, :], 128)
    near_c, near_s = trig((2 * np.arange(16)[:, None] + 1) * n[None, :], 2 * CYCLE_READINGS)
    return fine_c, fine_s, coarse_c, coarse_s, far_c, far_s, near_c, near_s


def split(x):
    high = x.astype(BF16)
    return high, (x - high.astype(F32)).astype(BF16)


def product(x, high_table, low_table):
    m = x.shape[0]
    high, low = split(x)
    both = jnp.dot(jnp.concatenate([high, low], axis=0), high_table, preferred_element_type=F32)
    return both[:m] + both[m:] + jnp.dot(high, low_table, preferred_element_type=F32)


def kernel(
    src, label, prior, attenuation, drain, diffusivity,
    fine_c, fine_s, coarse_c, coarse_s, far_c, far_s, near_c, near_s,
    field, later,
    S, VA, VB, M, R, Y, W,
    synth_c, synth_s, anal_c, anal_s,
    factors_fine, factors_coarse, factors_far, factors_near,
    early, late, heat_rows, heat_out, wide,
    load_sem, row_send, row_recv, col_send, col_recv, corner_send, corner_recv,
    early_send, early_recv, late_send, late_recv,
    one_send, one_recv, two_send, two_recv, heat_send, heat_recv,
):
    harm = lax.axis_index("harm")
    tx = lax.axis_index("tx")
    ty = lax.axis_index("ty")
    half = harm // 2
    core = harm % 2
    far_ty = (ty + 4) % TY
    wrapped = (ty + 4) // TY

    def remote(a, b, send, recv, device):
        return pltpu.make_async_remote_copy(
            src_ref=a, dst_ref=b, send_sem=send, recv_sem=recv,
            device_id=device, device_id_type=pl.DeviceIdType.MESH,
        )

    def owner(row):
        return (2 * ((row // 2 + wrapped) % 2) + row % 2, tx, far_ty)

    own_row = 2 * ((half + (far_ty + 4) // TY) % 2) + core

    def inside(dy, dx):
        ok = None
        for at, step, count in ((tx, dy, TX), (ty, dx, TY)):
            if step == 0:
                continue
            one = at > 0 if step < 0 else at < count - 1
            ok = one if ok is None else jnp.logical_and(ok, one)
        return ok

    loads = []
    for i, (a, b) in enumerate((
        (fine_c, factors_fine.at[0]), (fine_s, factors_fine.at[1]),
        (coarse_c, factors_coarse.at[0]), (coarse_s, factors_coarse.at[1]),
        (far_c, factors_far.at[0]), (far_s, factors_far.at[1]),
        (near_c, factors_near.at[0]), (near_s, factors_near.at[1]),
    )):
        copy = pltpu.make_async_copy(a, b, load_sem.at[i])
        copy.start()
        loads.append(copy)

    @pl.when(tx == 0)
    def _():
        S[:, 0:4] = jnp.zeros((2, 4, COLS + 2 * PAD, OWN), F32)
        for dx in range(3):
            early[0, dx] = jnp.zeros((3, ROWS, COLS), F32)
            late[0, dx] = jnp.zeros((ROWS, COLS), F32)

    @pl.when(tx == TX - 1)
    def _():
        S[:, 8:12] = jnp.zeros((2, 4, COLS + 2 * PAD, OWN), F32)
        for dx in range(3):
            early[2, dx] = jnp.zeros((3, ROWS, COLS), F32)
            late[2, dx] = jnp.zeros((ROWS, COLS), F32)

    @pl.when(ty == 0)
    def _():
        S[:, :, 8:16] = jnp.zeros((2, 12, 8, OWN), F32)
        for dy in range(3):
            early[dy, 0] = jnp.zeros((3, ROWS, COLS), F32)
            late[dy, 0] = jnp.zeros((ROWS, COLS), F32)

    @pl.when(ty == TY - 1)
    def _():
        S[:, :, PAD + COLS:PAD + COLS + 8] = jnp.zeros((2, 12, 8, OWN), F32)
        for dy in range(3):
            early[dy, 2] = jnp.zeros((3, ROWS, COLS), F32)
            late[dy, 2] = jnp.zeros((ROWS, COLS), F32)

    barrier = pltpu.get_barrier_semaphore()
    for dy, dx in AROUND:
        @pl.when(inside(dy, dx))
        def _():
            pl.semaphore_signal(barrier, inc=1, device_id=(harm, tx + dy, ty + dx), device_id_type=pl.DeviceIdType.MESH)
    for j in range(4):
        pl.semaphore_signal(barrier, inc=1, device_id=(j, tx, far_ty), device_id_type=pl.DeviceIdType.MESH)

    kinds = label[...]
    conduct = jnp.zeros((ROWS, COLS), F32)
    perfuse = jnp.zeros((ROWS, COLS), F32)
    absorb = jnp.zeros((ROWS, COLS), F32)
    for k in range(8):
        hit = kinds == k
        conduct = jnp.where(hit, diffusivity[k], conduct)
        perfuse = jnp.where(hit, drain[k], perfuse)
        absorb = jnp.where(hit, attenuation[k], absorb)
    early[1, 1, 0] = prior[...]
    early[1, 1, 1] = conduct
    early[1, 1, 2] = perfuse

    def edges(at, count):
        return jnp.where(at == 0, 1, 0) + jnp.where(at == count - 1, 1, 0)

    pl.semaphore_wait(barrier, (3 - edges(tx, TX)) * (3 - edges(ty, TY)) + 3)

    def row_copy(side, c):
        return remote(
            src.at[:, :, pl.ds(c * WIDTH, WIDTH), :],
            S.at[:, pl.ds(8 * side, 4), pl.ds(PAD + c * WIDTH, WIDTH), :],
            row_send.at[side, c], row_recv.at[side, c], (harm, tx + 1 - 2 * side, ty),
        )

    def col_copy(side):
        return remote(
            src.at[:, :, pl.ds(0 if side else COLS - 8, 8), :],
            S.at[:, 4:8, pl.ds(PAD + COLS if side else PAD - 8, 8), :],
            col_send.at[side], col_recv.at[side], (harm, tx, ty + 1 - 2 * side),
        )

    def corner_copy(side, vertical):
        at = PAD + COLS if side else PAD - 8
        return remote(
            S.at[:, 4:8, pl.ds(at, 8), :],
            S.at[:, pl.ds(8 * vertical, 4), pl.ds(at, 8), :],
            corner_send.at[side, vertical], corner_recv.at[side, vertical],
            (harm, tx + 1 - 2 * vertical, ty),
        )

    def to_side(side):
        return tx < TX - 1 if side == 0 else tx > 0

    def from_side(side):
        return tx > 0 if side == 0 else tx < TX - 1

    def to_col(side):
        return ty < TY - 1 if side == 0 else ty > 0

    def from_col(side):
        return ty > 0 if side == 0 else ty < TY - 1

    for side in (0, 1):
        @pl.when(to_col(side))
        def _():
            col_copy(side).start()
    for c in range(CHUNKS):
        for side in (0, 1):
            @pl.when(to_side(side))
            def _():
                row_copy(side, c).start()

    def early_copy(dy, dx):
        slot = 3 * (dy + 1) + dx + 1
        return remote(
            early.at[1, 1], early.at[1 - dy, 1 - dx], early_send.at[slot], early_recv.at[8 - slot],
            (harm, tx + dy, ty + dx),
        )

    def late_copy(dy, dx):
        slot = 3 * (dy + 1) + dx + 1
        return remote(
            late.at[1, 1], late.at[1 - dy, 1 - dx], late_send.at[slot], late_recv.at[8 - slot],
            (harm, tx + dy, ty + dx),
        )

    for dy, dx in AROUND:
        @pl.when(inside(dy, dx))
        def _():
            early_copy(dy, dx).start()

    for p in range(2):
        for row in range(ROWS):
            S[p, 4 + row, PAD:PAD + COLS, :] = src[p, row]

    lane = lax.broadcasted_iota(jnp.int32, (1, OWN), 1)
    gain = diffraction_gain / (harm * OWN + lane + 1).astype(F32)

    def row_inside(row):
        at = tx * ROWS + row - 4
        return jnp.where(jnp.logical_and(at >= 0, at < TX * ROWS), 1.0, 0.0).astype(F32)

    def stencil(c):
        base = c * WIDTH
        for k, source, target in ((1, S, VA), (2, VA, VB), (3, VB, VA), (4, VA, M)):
            low, count = (PAD, WIDTH) if k == 4 else (8, WIDTH + 16)
            shift = base if k == 1 else 0
            at = ty * COLS + base + low - PAD + lax.broadcasted_iota(jnp.int32, (count, OWN), 0)
            valid = jnp.logical_and(at >= 0, at < TY * COLS)
            g = jnp.where(valid, gain * (1.0 / (5 - k)), 0.0)

            def one_row(row, carry):
                gr = g * row_inside(row)
                laps = []
                for p in range(2):
                    center = source[p, row, pl.ds(shift + low, count), :]
                    laps.append(
                        source[p, row + 1, pl.ds(shift + low, count), :]
                        + source[p, row - 1, pl.ds(shift + low, count), :]
                        + source[p, row, pl.ds(shift + low + 1, count), :]
                        + source[p, row, pl.ds(shift + low - 1, count), :]
                        - 4.0 * center
                    )
                real = S[0, row, pl.ds(base + low, count), :] - gr * laps[1]
                imag = S[1, row, pl.ds(base + low, count), :] + gr * laps[0]
                if k == 4:
                    target[0, row - 4, pl.ds(base, count), :] = real
                    target[1, row - 4, pl.ds(base, count), :] = imag
                else:
                    target[0, row, pl.ds(low, count), :] = real
                    target[1, row, pl.ds(low, count), :] = imag
                return carry

            lax.fori_loop(k, 12 - k, one_row, 0)

    def one_copy(c, row):
        return remote(
            M.at[:, row, pl.ds(c * WIDTH, WIDTH), :],
            R.at[harm, :, pl.ds(c * WIDTH, WIDTH), :],
            one_send.at[c, row], one_recv.at[c, harm], owner(row),
        )

    def one_arrival(c, j):
        return remote(
            M.at[:, 0, pl.ds(c * WIDTH, WIDTH), :],
            R.at[j, :, pl.ds(c * WIDTH, WIDTH), :],
            one_send.at[c, 0], one_recv.at[c, j], (j, tx, far_ty),
        )

    def two_copy(c, j):
        return remote(
            Y.at[j, :, pl.ds(c * WIDTH, WIDTH), :],
            field.at[own_row, :, pl.ds(c * WIDTH, WIDTH), :],
            two_send.at[c, j], two_recv.at[c, own_row], (j, tx, far_ty),
        )

    def two_arrival(c, row):
        return remote(
            Y.at[0, :, pl.ds(c * WIDTH, WIDTH), :],
            field.at[row, :, pl.ds(c * WIDTH, WIDTH), :],
            two_send.at[c, 0], two_recv.at[c, row], owner(row),
        )

    def wait_rows(c):
        for side in (0, 1):
            @pl.when(from_side(side))
            def _():
                row_copy(side, c).wait_recv()

    def forward(side):
        @pl.when(from_col(side))
        def _():
            col_copy(side).wait_recv()
            for vertical in (0, 1):
                @pl.when(to_side(vertical))
                def _():
                    corner_copy(side, vertical).start()

    def wait_corners(side):
        @pl.when(from_col(side))
        def _():
            for vertical in (0, 1):
                @pl.when(from_side(vertical))
                def _():
                    corner_copy(side, vertical).wait_recv()

    def build_tables():
        for copy in loads:
            copy.wait()

        def by_time(i, carry):
            rows = pl.ds(pl.multiple_of(i * 16, 16), 16)
            fc = factors_fine[0, rows, :]
            fs = factors_fine[1, rows, :]
            for a in range(8):
                ac = factors_coarse[0, a]
                as_ = factors_coarse[1, a]
                for table, value in ((synth_c, ac * fc - as_ * fs), (synth_s, as_ * fc + ac * fs)):
                    high, low = split(value)
                    table[0, rows, a * 128:(a + 1) * 128] = high
                    table[1, rows, a * 128:(a + 1) * 128] = low
            return carry

        lax.fori_loop(0, HARMONICS // 16, by_time, 0)

        def by_harmonic(a, carry):
            rows = pl.ds(pl.multiple_of(a * 16, 16), 16)
            ac = factors_far[0, pl.ds(a, 1), :]
            as_ = factors_far[1, pl.ds(a, 1), :]
            nc = factors_near[0]
            ns = factors_near[1]
            for table, value in ((anal_c, ac * nc - as_ * ns), (anal_s, as_ * nc + ac * ns)):
                high, low = split(value)
                table[0, rows, :] = high
                table[1, rows, :] = low
            return carry

        lax.fori_loop(0, HALF // 16, by_harmonic, 0)

    forward(0)
    forward(1)
    wait_rows(0)
    wait_corners(0)
    for c in range(CHUNKS):
        if c + 1 < CHUNKS:
            wait_rows(c + 1)
        else:
            wait_corners(1)
        stencil(c)
        for row in range(ROWS):
            one_copy(c, row).start()
    build_tables()

    numbers = (lax.broadcasted_iota(jnp.int32, (1, HARMONICS), 1) + 1).astype(F32)
    scale = 2.0 * math.sqrt(HARMONICS) / CYCLE_READINGS / HARMONICS
    real_factor = numbers * (nonlinear_gain / HARMONICS * 4.0 * scale)
    imag_factor = numbers * (nonlinear_gain / HARMONICS * 2.0 * scale)

    def nonlinear(c, carry):
        for j in range(4):
            one_arrival(c, j).wait_recv()
        cols = pl.ds(pl.multiple_of(c * WIDTH, WIDTH), WIDTH)
        real = jnp.concatenate([R[j, 0, cols, :] for j in range(4)], axis=1)
        imag = jnp.concatenate([R[j, 1, cols, :] for j in range(4)], axis=1)
        even = product(real, synth_c[0], synth_c[1])
        odd = product(imag, synth_s[0], synth_s[1])
        cosine = product(even * even + odd * odd, anal_c[0], anal_c[1])
        sine = product(even * odd, anal_s[0], anal_s[1])
        real = real - real_factor * sine
        imag = imag + imag_factor * cosine
        weighted = numbers * (real * real + imag * imag)
        W[cols, :] = weighted[:, 0:128] + weighted[:, 128:256] + weighted[:, 256:384] + weighted[:, 384:512]
        for j in range(4):
            Y[j, 0, cols, :] = real[:, 128 * j:128 * (j + 1)]
            Y[j, 1, cols, :] = imag[:, 128 * j:128 * (j + 1)]
        for j in range(4):
            two_copy(c, j).start()
        return carry

    lax.fori_loop(0, CHUNKS, nonlinear, 0)

    heat_out[...] = lax.dot_general(
        jnp.ones((8, OWN), F32), W[...], (((1,), (1,)), ((), ())),
        precision=lax.Precision.HIGHEST, preferred_element_type=F32,
    )[0:1]

    def heat_copy(j):
        return remote(heat_out, heat_rows.at[own_row], heat_send.at[j], heat_recv.at[own_row], (j, tx, far_ty))

    for j in range(4):
        heat_copy(j).start()
    for row in range(ROWS):
        remote(heat_out, heat_rows.at[row], heat_send.at[0], heat_recv.at[row], owner(row)).wait_recv()
    for row in range(ROWS):
        late[1, 1, row:row + 1, :] = absorb[row:row + 1] * heat_rows[row] / float(HARMONICS * HARMONICS)
    for dy, dx in AROUND:
        @pl.when(inside(dy, dx))
        def _():
            late_copy(dy, dx).start()
    for dy, dx in AROUND:
        @pl.when(inside(dy, dx))
        def _():
            early_copy(-dy, -dx).wait_recv()
    for dy, dx in AROUND:
        @pl.when(inside(dy, dx))
        def _():
            late_copy(-dy, -dx).wait_recv()
    for dy in range(3):
        for dx in range(3):
            rows = slice(4 * dy, 4 * dy + 4)
            cols = slice(128 * dx, 128 * dx + 128)
            for k in range(3):
                wide[k, rows, cols] = early[dy, dx, k]
            wide[3, rows, cols] = late[dy, dx]
    for k in range(4):
        wide[k, 12:16, :] = jnp.zeros((4, 3 * COLS), F32)
    temperature = wide[0]
    wide_conduct = wide[1]
    wide_perfuse = wide[2]
    wide_deposit = wide[3]
    for _ in range(4):
        lap = (
            pltpu.roll(temperature, 15, 0) + pltpu.roll(temperature, 1, 0)
            + pltpu.roll(temperature, 3 * COLS - 1, 1) + pltpu.roll(temperature, 1, 1)
            - 4.0 * temperature
        )
        temperature = temperature + wide_conduct * lap - wide_perfuse * temperature + wide_deposit
    wide[0] = temperature
    later[...] = wide[0, 4:8, COLS:2 * COLS]

    for side in (0, 1):
        @pl.when(to_col(side))
        def _():
            col_copy(side).wait_send()
        for c in range(CHUNKS):
            @pl.when(to_side(side))
            def _():
                row_copy(side, c).wait_send()

        @pl.when(from_col(side))
        def _():
            for vertical in (0, 1):
                @pl.when(to_side(vertical))
                def _():
                    corner_copy(side, vertical).wait_send()
    for dy, dx in AROUND:
        @pl.when(inside(dy, dx))
        def _():
            early_copy(dy, dx).wait_send()
            late_copy(dy, dx).wait_send()
    for j in range(4):
        heat_copy(j).wait_send()
    for c in range(CHUNKS):
        for j in range(4):
            one_copy(c, j).wait_send()
            two_copy(c, j).wait_send()
            two_arrival(c, j).wait_recv()


def solution(mesh):
    factors = table_factors()

    def body(wave, lens, label, prior, attenuation, drain, diffusivity):
        weight = 0.25 + 0.75 * lens.astype(F32)
        src = jnp.transpose(wave * weight, (0, 2, 3, 1))
        vmem = pl.BlockSpec(memory_space=pltpu.VMEM)
        smem = pl.BlockSpec(memory_space=pltpu.SMEM)
        hbm = pl.BlockSpec(memory_space=pl.ANY)
        dma = pltpu.SemaphoreType.DMA
        field, later = pl.pallas_call(
            kernel,
            out_shape=(
                jax.ShapeDtypeStruct((ROWS, 2, COLS, OWN), F32),
                jax.ShapeDtypeStruct((ROWS, COLS), F32),
            ),
            in_specs=[vmem, vmem, vmem, smem, smem, smem] + [hbm] * 8,
            out_specs=(hbm, vmem),
            scratch_shapes=[
                pltpu.VMEM((2, 12, COLS + 2 * PAD, OWN), F32),
                pltpu.VMEM((2, 12, WIDTH + 2 * PAD, OWN), F32),
                pltpu.VMEM((2, 12, WIDTH + 2 * PAD, OWN), F32),
                pltpu.VMEM((2, ROWS, COLS, OWN), F32),
                pltpu.VMEM((4, 2, COLS, OWN), F32),
                pltpu.VMEM((4, 2, COLS, OWN), F32),
                pltpu.VMEM((COLS, OWN), F32),
                pltpu.VMEM((2, HARMONICS, HALF), BF16),
                pltpu.VMEM((2, HARMONICS, HALF), BF16),
                pltpu.VMEM((2, HALF, HARMONICS), BF16),
                pltpu.VMEM((2, HALF, HARMONICS), BF16),
                pltpu.VMEM((2, HARMONICS, 128), F32),
                pltpu.VMEM((2, 8, 16, 128), F32),
                pltpu.VMEM((2, 64, HARMONICS), F32),
                pltpu.VMEM((2, 16, HARMONICS), F32),
                pltpu.VMEM((3, 3, 3, ROWS, COLS), F32),
                pltpu.VMEM((3, 3, ROWS, COLS), F32),
                pltpu.VMEM((ROWS, 1, COLS), F32),
                pltpu.VMEM((1, COLS), F32),
                pltpu.VMEM((4, 16, 3 * COLS), F32),
                dma((8,)), dma((2, CHUNKS)), dma((2, CHUNKS)), dma((2,)), dma((2,)), dma((2, 2)), dma((2, 2)),
                dma((9,)), dma((9,)), dma((9,)), dma((9,)),
                dma((CHUNKS, 4)), dma((CHUNKS, 4)), dma((CHUNKS, 4)), dma((CHUNKS, 4)), dma((4,)), dma((4,)),
            ],
            compiler_params=pltpu.CompilerParams(
                collective_id=0, has_side_effects=True, vmem_limit_bytes=48 << 20
            ),
            name="march",
        )(src, label, prior, attenuation, drain, diffusivity, *[jnp.asarray(f) for f in factors])
        return jnp.transpose(field, (1, 3, 0, 2)), later

    in_specs = (P(None, "harm", "tx", "ty"), P("tx", "ty"), P("tx", "ty"), P("tx", "ty"), P(), P(), P())
    out_specs = (P(None, "harm", "tx", "ty"), P("tx", "ty"))
    return jax.shard_map(body, mesh=mesh, in_specs=in_specs, out_specs=out_specs, check_vma=False)
```

```python
import math

import jax
import jax.numpy as jnp
import numpy as np
from jax import lax
from jax.experimental import pallas as pl
from jax.experimental.pallas import tpu as pltpu
from jax.sharding import PartitionSpec as P

CYCLE_READINGS = 2048
HALF = CYCLE_READINGS // 2
HARMONICS = 512
OWN = 128
ROWS = 4
COLS = 128
CHUNKS = 8
WIDTH = COLS // CHUNKS
ORDER = (1, 0, 2, 3, 4, 5, 6, 7)
PARTS = 4
PART = COLS // PARTS
PAD = 16
F32 = jnp.float32
BF16 = jnp.bfloat16

diffraction_gain = 0.3
nonlinear_gain = 0.3

TX = 16
TY = 8
AROUND = [(dy, dx) for dy in (-1, 0, 1) for dx in (-1, 0, 1) if (dy, dx) != (0, 0)]


def trig(product, period):
    angle = 2.0 * np.pi * (product % period) / period
    return np.cos(angle).astype(np.float32), np.sin(angle).astype(np.float32)


def table_factors():
    n = np.arange(1, HARMONICS + 1, dtype=np.int64)
    fine_c, fine_s = trig(n[:, None] * (2 * np.arange(128)[None, :] + 1), 2 * CYCLE_READINGS)
    coarse_c, coarse_s = trig(np.arange(8)[:, None] * np.arange(1, 17)[None, :], 16)
    coarse_c = np.repeat(coarse_c[:, :, None], 128, axis=2)
    coarse_s = np.repeat(coarse_s[:, :, None], 128, axis=2)
    far_c, far_s = trig(np.arange(64)[:, None] * n[None, :], 128)
    near_c, near_s = trig((2 * np.arange(16)[:, None] + 1) * n[None, :], 2 * CYCLE_READINGS)
    return fine_c, fine_s, coarse_c, coarse_s, far_c, far_s, near_c, near_s


def split(x):
    high = x.astype(BF16)
    return high, (x - high.astype(F32)).astype(BF16)


def product(x, high_table, low_table):
    m = x.shape[0]
    high, low = split(x)
    both = jnp.dot(jnp.concatenate([high, low], axis=0), high_table, preferred_element_type=F32)
    return both[:m] + both[m:] + jnp.dot(high, low_table, preferred_element_type=F32)


def kernel(
    wave, lens, label, prior, attenuation, drain, diffusivity,
    fine_c, fine_s, coarse_c, coarse_s, far_c, far_s, near_c, near_s,
    field, later,
    raw, S, VA, VB, M, R, Y, W,
    synth_c, synth_s, anal_c, anal_s,
    factors_fine, factors_coarse, factors_far, factors_near,
    early, late, heat_rows, heat_out, wide,
    raw_sem, load_sem, row_send, row_recv, col_send, col_recv, corner_send, corner_recv,
    early_send, early_recv, late_send, late_recv,
    one_send, one_recv, two_send, two_recv, heat_send, heat_recv,
):
    harm = lax.axis_index("harm")
    tx = lax.axis_index("tx")
    ty = lax.axis_index("ty")
    half = harm // 2
    core = harm % 2
    far_ty = (ty + 4) % TY
    wrapped = (ty + 4) // TY

    def remote(a, b, send, recv, device):
        return pltpu.make_async_remote_copy(
            src_ref=a, dst_ref=b, send_sem=send, recv_sem=recv,
            device_id=device, device_id_type=pl.DeviceIdType.MESH,
        )

    def owner(row):
        return (2 * ((row // 2 + wrapped) % 2) + row % 2, tx, far_ty)

    own_row = 2 * ((half + (far_ty + 4) // TY) % 2) + core

    def inside(dy, dx):
        ok = None
        for at, step, count in ((tx, dy, TX), (ty, dx, TY)):
            if step == 0:
                continue
            one = at > 0 if step < 0 else at < count - 1
            ok = one if ok is None else jnp.logical_and(ok, one)
        return ok

    raws = []
    for p in range(2):
        for row in range(ROWS):
            copy = pltpu.make_async_copy(wave.at[p, :, row, :], raw.at[p, row], raw_sem.at[p, row])
            copy.start()
            raws.append((p, row, copy))
    loads = []
    for i, (a, b) in enumerate((
        (fine_c, factors_fine.at[0]), (fine_s, factors_fine.at[1]),
        (coarse_c, factors_coarse.at[0]), (coarse_s, factors_coarse.at[1]),
        (far_c, factors_far.at[0]), (far_s, factors_far.at[1]),
        (near_c, factors_near.at[0]), (near_s, factors_near.at[1]),
    )):
        copy = pltpu.make_async_copy(a, b, load_sem.at[i])
        copy.start()
        loads.append(copy)

    @pl.when(tx == 0)
    def _():
        S[:, 0:4] = jnp.zeros((2, 4, COLS + 2 * PAD, OWN), F32)
        for dx in range(3):
            early[0, dx] = jnp.zeros((3, ROWS, COLS), F32)
            late[0, dx] = jnp.zeros((ROWS, COLS), F32)

    @pl.when(tx == TX - 1)
    def _():
        S[:, 8:12] = jnp.zeros((2, 4, COLS + 2 * PAD, OWN), F32)
        for dx in range(3):
            early[2, dx] = jnp.zeros((3, ROWS, COLS), F32)
            late[2, dx] = jnp.zeros((ROWS, COLS), F32)

    @pl.when(ty == 0)
    def _():
        S[:, :, 8:16] = jnp.zeros((2, 12, 8, OWN), F32)
        for dy in range(3):
            early[dy, 0] = jnp.zeros((3, ROWS, COLS), F32)
            late[dy, 0] = jnp.zeros((ROWS, COLS), F32)

    @pl.when(ty == TY - 1)
    def _():
        S[:, :, PAD + COLS:PAD + COLS + 8] = jnp.zeros((2, 12, 8, OWN), F32)
        for dy in range(3):
            early[dy, 2] = jnp.zeros((3, ROWS, COLS), F32)
            late[dy, 2] = jnp.zeros((ROWS, COLS), F32)

    barrier = pltpu.get_barrier_semaphore()
    for dy, dx in AROUND:
        @pl.when(inside(dy, dx))
        def _():
            pl.semaphore_signal(barrier, inc=1, device_id=(harm, tx + dy, ty + dx), device_id_type=pl.DeviceIdType.MESH)
    for j in range(4):
        pl.semaphore_signal(barrier, inc=1, device_id=(j, tx, far_ty), device_id_type=pl.DeviceIdType.MESH)

    weight = 0.25 + 0.75 * lens[...].astype(F32)
    for p, row, copy in raws:
        copy.wait()
        S[p, 4 + row, PAD:PAD + COLS, :] = jnp.transpose(raw[p, row] * weight[row:row + 1, :])

    kinds = label[...]
    conduct = jnp.zeros((ROWS, COLS), F32)
    perfuse = jnp.zeros((ROWS, COLS), F32)
    absorb = jnp.zeros((ROWS, COLS), F32)
    for k in range(8):
        hit = kinds == k
        conduct = jnp.where(hit, diffusivity[k], conduct)
        perfuse = jnp.where(hit, drain[k], perfuse)
        absorb = jnp.where(hit, attenuation[k], absorb)
    early[1, 1, 0] = prior[...]
    early[1, 1, 1] = conduct
    early[1, 1, 2] = perfuse

    def edges(at, count):
        return jnp.where(at == 0, 1, 0) + jnp.where(at == count - 1, 1, 0)

    pl.semaphore_wait(barrier, (3 - edges(tx, TX)) * (3 - edges(ty, TY)) + 3)

    def row_copy(side, c):
        return remote(
            S.at[:, 4:8, pl.ds(PAD + c * WIDTH, WIDTH), :],
            S.at[:, pl.ds(8 * side, 4), pl.ds(PAD + c * WIDTH, WIDTH), :],
            row_send.at[side, c], row_recv.at[side, c], (harm, tx + 1 - 2 * side, ty),
        )

    def col_copy(side):
        return remote(
            S.at[:, 4:8, pl.ds(PAD if side else PAD + COLS - 8, 8), :],
            S.at[:, 4:8, pl.ds(PAD + COLS if side else PAD - 8, 8), :],
            col_send.at[side], col_recv.at[side], (harm, tx, ty + 1 - 2 * side),
        )

    def corner_copy(side, vertical):
        at = PAD + COLS if side else PAD - 8
        return remote(
            S.at[:, 4:8, pl.ds(at, 8), :],
            S.at[:, pl.ds(8 * vertical, 4), pl.ds(at, 8), :],
            corner_send.at[side, vertical], corner_recv.at[side, vertical],
            (harm, tx + 1 - 2 * vertical, ty),
        )

    def to_side(side):
        return tx < TX - 1 if side == 0 else tx > 0

    def from_side(side):
        return tx > 0 if side == 0 else tx < TX - 1

    def to_col(side):
        return ty < TY - 1 if side == 0 else ty > 0

    def from_col(side):
        return ty > 0 if side == 0 else ty < TY - 1

    for side in (0, 1):
        @pl.when(to_col(side))
        def _():
            col_copy(side).start()
    def start_rows(c):
        for side in (0, 1):
            @pl.when(to_side(side))
            def _():
                row_copy(side, c).start()

    for c in range(3):
        start_rows(c)

    def early_copy(dy, dx):
        slot = 3 * (dy + 1) + dx + 1
        return remote(
            early.at[1, 1], early.at[1 - dy, 1 - dx], early_send.at[slot], early_recv.at[8 - slot],
            (harm, tx + dy, ty + dx),
        )

    def late_copy(dy, dx):
        slot = 3 * (dy + 1) + dx + 1
        return remote(
            late.at[1, 1], late.at[1 - dy, 1 - dx], late_send.at[slot], late_recv.at[8 - slot],
            (harm, tx + dy, ty + dx),
        )

    for dy, dx in AROUND:
        @pl.when(inside(dy, dx))
        def _():
            early_copy(dy, dx).start()

    lane = lax.broadcasted_iota(jnp.int32, (1, OWN), 1)
    gain = diffraction_gain / (harm * OWN + lane + 1).astype(F32)

    def row_inside(row):
        at = tx * ROWS + row - 4
        return jnp.where(jnp.logical_and(at >= 0, at < TX * ROWS), 1.0, 0.0).astype(F32)

    def stencil(c):
        base = c * WIDTH
        for k, source, target in ((1, S, VA), (2, VA, VB), (3, VB, VA), (4, VA, M)):
            low, count = (PAD, WIDTH) if k == 4 else (8, WIDTH + 16)
            shift = base if k == 1 else 0
            at = ty * COLS + base + low - PAD + lax.broadcasted_iota(jnp.int32, (count, OWN), 0)
            valid = jnp.logical_and(at >= 0, at < TY * COLS)
            g = jnp.where(valid, gain * (1.0 / (5 - k)), 0.0)

            def one_row(row, carry):
                gr = g * row_inside(row)
                laps = []
                for p in range(2):
                    center = source[p, row, pl.ds(shift + low, count), :]
                    laps.append(
                        source[p, row + 1, pl.ds(shift + low, count), :]
                        + source[p, row - 1, pl.ds(shift + low, count), :]
                        + source[p, row, pl.ds(shift + low + 1, count), :]
                        + source[p, row, pl.ds(shift + low - 1, count), :]
                        - 4.0 * center
                    )
                real = S[0, row, pl.ds(base + low, count), :] - gr * laps[1]
                imag = S[1, row, pl.ds(base + low, count), :] + gr * laps[0]
                if k == 4:
                    target[0, row - 4, pl.ds(base, count), :] = real
                    target[1, row - 4, pl.ds(base, count), :] = imag
                else:
                    target[0, row, pl.ds(low, count), :] = real
                    target[1, row, pl.ds(low, count), :] = imag
                return carry

            lax.fori_loop(k, 12 - k, one_row, 0)

    def one_copy(c, row):
        return remote(
            M.at[:, row, pl.ds(c * WIDTH, WIDTH), :],
            R.at[harm, :, pl.ds(c * WIDTH, WIDTH), :],
            one_send.at[c, row], one_recv.at[c, harm], owner(row),
        )

    def one_arrival(c, j):
        return remote(
            M.at[:, 0, pl.ds(c * WIDTH, WIDTH), :],
            R.at[j, :, pl.ds(c * WIDTH, WIDTH), :],
            one_send.at[c, 0], one_recv.at[c, j], (j, tx, far_ty),
        )

    def two_copy(c, j):
        return remote(
            Y.at[j, :, pl.ds(c * PART, PART), :],
            field.at[own_row, :, pl.ds(c * PART, PART), :],
            two_send.at[c, j], two_recv.at[c, own_row], (j, tx, far_ty),
        )

    def two_arrival(c, row):
        return remote(
            Y.at[0, :, pl.ds(c * PART, PART), :],
            field.at[row, :, pl.ds(c * PART, PART), :],
            two_send.at[c, 0], two_recv.at[c, row], owner(row),
        )

    def wait_rows(c):
        for side in (0, 1):
            @pl.when(from_side(side))
            def _():
                row_copy(side, c).wait_recv()

    def forward(side):
        @pl.when(from_col(side))
        def _():
            col_copy(side).wait_recv()
            for vertical in (0, 1):
                @pl.when(to_side(vertical))
                def _():
                    corner_copy(side, vertical).start()

    def wait_corners(side):
        @pl.when(from_col(side))
        def _():
            for vertical in (0, 1):
                @pl.when(from_side(vertical))
                def _():
                    corner_copy(side, vertical).wait_recv()

    def build_tables():
        for copy in loads:
            copy.wait()

        def by_time(i, carry):
            rows = pl.ds(pl.multiple_of(i * 16, 16), 16)
            fc = factors_fine[0, rows, :]
            fs = factors_fine[1, rows, :]
            for a in range(8):
                ac = factors_coarse[0, a]
                as_ = factors_coarse[1, a]
                for table, value in ((synth_c, ac * fc - as_ * fs), (synth_s, as_ * fc + ac * fs)):
                    high, low = split(value)
                    table[0, rows, a * 128:(a + 1) * 128] = high
                    table[1, rows, a * 128:(a + 1) * 128] = low
            return carry

        lax.fori_loop(0, HARMONICS // 16, by_time, 0)

        def by_harmonic(a, carry):
            rows = pl.ds(pl.multiple_of(a * 16, 16), 16)
            ac = factors_far[0, pl.ds(a, 1), :]
            as_ = factors_far[1, pl.ds(a, 1), :]
            nc = factors_near[0]
            ns = factors_near[1]
            for table, value in ((anal_c, ac * nc - as_ * ns), (anal_s, as_ * nc + ac * ns)):
                high, low = split(value)
                table[0, rows, :] = high
                table[1, rows, :] = low
            return carry

        lax.fori_loop(0, HALF // 16, by_harmonic, 0)

    forward(0)
    for c in range(3, 6):
        start_rows(c)
    forward(1)
    for c in range(6, CHUNKS):
        start_rows(c)
    arrived = 0
    for c in ORDER:
        while arrived < min(c + 2, CHUNKS):
            wait_rows(arrived)
            arrived += 1
        if c == 0:
            wait_corners(0)
        if c == CHUNKS - 1:
            wait_corners(1)
        stencil(c)
        for row in range(ROWS):
            one_copy(c, row).start()
    build_tables()

    numbers = (lax.broadcasted_iota(jnp.int32, (1, HARMONICS), 1) + 1).astype(F32)
    scale = 2.0 * math.sqrt(HARMONICS) / CYCLE_READINGS / HARMONICS
    real_factor = numbers * (nonlinear_gain / HARMONICS * 4.0 * scale)
    imag_factor = numbers * (nonlinear_gain / HARMONICS * 2.0 * scale)

    def nonlinear(c, carry):
        for k in range(PART // WIDTH):
            for j in range(4):
                one_arrival(c * (PART // WIDTH) + k, j).wait_recv()
        cols = pl.ds(pl.multiple_of(c * PART, PART), PART)
        real = jnp.concatenate([R[j, 0, cols, :] for j in range(4)], axis=1)
        imag = jnp.concatenate([R[j, 1, cols, :] for j in range(4)], axis=1)
        even = product(real, synth_c[0], synth_c[1])
        odd = product(imag, synth_s[0], synth_s[1])
        cosine = product(even * even + odd * odd, anal_c[0], anal_c[1])
        sine = product(even * odd, anal_s[0], anal_s[1])
        real = real - real_factor * sine
        imag = imag + imag_factor * cosine
        weighted = numbers * (real * real + imag * imag)
        W[cols, :] = weighted[:, 0:128] + weighted[:, 128:256] + weighted[:, 256:384] + weighted[:, 384:512]
        for j in range(4):
            Y[j, 0, cols, :] = real[:, 128 * j:128 * (j + 1)]
            Y[j, 1, cols, :] = imag[:, 128 * j:128 * (j + 1)]

        @pl.when(c < PARTS - 1)
        def _():
            for j in range(4):
                two_copy(c, j).start()

        return carry

    lax.fori_loop(0, PARTS, nonlinear, 0)

    heat_out[...] = lax.dot_general(
        jnp.ones((8, OWN), F32), W[...], (((1,), (1,)), ((), ())),
        precision=lax.Precision.HIGHEST, preferred_element_type=F32,
    )[0:1]

    def heat_copy(j):
        return remote(heat_out, heat_rows.at[own_row], heat_send.at[j], heat_recv.at[own_row], (j, tx, far_ty))

    for j in range(4):
        heat_copy(j).start()
    for j in range(4):
        two_copy(PARTS - 1, j).start()
    for row in range(ROWS):
        remote(heat_out, heat_rows.at[row], heat_send.at[0], heat_recv.at[row], owner(row)).wait_recv()
    for row in range(ROWS):
        late[1, 1, row:row + 1, :] = absorb[row:row + 1] * heat_rows[row] / float(HARMONICS * HARMONICS)
    for dy, dx in AROUND:
        @pl.when(inside(dy, dx))
        def _():
            late_copy(dy, dx).start()
    for dy, dx in AROUND:
        @pl.when(inside(dy, dx))
        def _():
            early_copy(-dy, -dx).wait_recv()
    for dy, dx in AROUND:
        @pl.when(inside(dy, dx))
        def _():
            late_copy(-dy, -dx).wait_recv()
    for dy in range(3):
        for dx in range(3):
            rows = slice(4 * dy, 4 * dy + 4)
            cols = slice(128 * dx, 128 * dx + 128)
            for k in range(3):
                wide[k, rows, cols] = early[dy, dx, k]
            wide[3, rows, cols] = late[dy, dx]
    for k in range(4):
        wide[k, 12:16, :] = jnp.zeros((4, 3 * COLS), F32)
    temperature = wide[0]
    wide_conduct = wide[1]
    wide_perfuse = wide[2]
    wide_deposit = wide[3]
    for _ in range(4):
        lap = (
            pltpu.roll(temperature, 15, 0) + pltpu.roll(temperature, 1, 0)
            + pltpu.roll(temperature, 3 * COLS - 1, 1) + pltpu.roll(temperature, 1, 1)
            - 4.0 * temperature
        )
        temperature = temperature + wide_conduct * lap - wide_perfuse * temperature + wide_deposit
    wide[0] = temperature
    later[...] = wide[0, 4:8, COLS:2 * COLS]

    for side in (0, 1):
        @pl.when(to_col(side))
        def _():
            col_copy(side).wait_send()
        for c in range(CHUNKS):
            @pl.when(to_side(side))
            def _():
                row_copy(side, c).wait_send()

        @pl.when(from_col(side))
        def _():
            for vertical in (0, 1):
                @pl.when(to_side(vertical))
                def _():
                    corner_copy(side, vertical).wait_send()
    for dy, dx in AROUND:
        @pl.when(inside(dy, dx))
        def _():
            early_copy(dy, dx).wait_send()
            late_copy(dy, dx).wait_send()
    for j in range(4):
        heat_copy(j).wait_send()
    for c in range(CHUNKS):
        for j in range(4):
            one_copy(c, j).wait_send()
    for c in range(PARTS):
        for j in range(4):
            two_copy(c, j).wait_send()
            two_arrival(c, j).wait_recv()


def solution(mesh):
    factors = table_factors()

    def body(wave, lens, label, prior, attenuation, drain, diffusivity):
        vmem = pl.BlockSpec(memory_space=pltpu.VMEM)
        smem = pl.BlockSpec(memory_space=pltpu.SMEM)
        hbm = pl.BlockSpec(memory_space=pltpu.HBM)
        anywhere = pl.BlockSpec(memory_space=pl.ANY)
        dma = pltpu.SemaphoreType.DMA
        field, later = pl.pallas_call(
            kernel,
            out_shape=(
                jax.ShapeDtypeStruct((ROWS, 2, COLS, OWN), F32),
                jax.ShapeDtypeStruct((ROWS, COLS), F32),
            ),
            in_specs=[hbm, vmem, vmem, vmem, smem, smem, smem] + [hbm] * 8,
            out_specs=(anywhere, vmem),
            scratch_shapes=[
                pltpu.VMEM((2, ROWS, OWN, COLS), F32),
                pltpu.VMEM((2, 12, COLS + 2 * PAD, OWN), F32),
                pltpu.VMEM((2, 12, WIDTH + 2 * PAD, OWN), F32),
                pltpu.VMEM((2, 12, WIDTH + 2 * PAD, OWN), F32),
                pltpu.VMEM((2, ROWS, COLS, OWN), F32),
                pltpu.VMEM((4, 2, COLS, OWN), F32),
                pltpu.VMEM((4, 2, COLS, OWN), F32),
                pltpu.VMEM((COLS, OWN), F32),
                pltpu.VMEM((2, HARMONICS, HALF), BF16),
                pltpu.VMEM((2, HARMONICS, HALF), BF16),
                pltpu.VMEM((2, HALF, HARMONICS), BF16),
                pltpu.VMEM((2, HALF, HARMONICS), BF16),
                pltpu.VMEM((2, HARMONICS, 128), F32),
                pltpu.VMEM((2, 8, 16, 128), F32),
                pltpu.VMEM((2, 64, HARMONICS), F32),
                pltpu.VMEM((2, 16, HARMONICS), F32),
                pltpu.VMEM((3, 3, 3, ROWS, COLS), F32),
                pltpu.VMEM((3, 3, ROWS, COLS), F32),
                pltpu.VMEM((ROWS, 1, COLS), F32),
                pltpu.VMEM((1, COLS), F32),
                pltpu.VMEM((4, 16, 3 * COLS), F32),
                dma((2, ROWS)), dma((8,)), dma((2, CHUNKS)), dma((2, CHUNKS)), dma((2,)), dma((2,)), dma((2, 2)), dma((2, 2)),
                dma((9,)), dma((9,)), dma((9,)), dma((9,)),
                dma((CHUNKS, 4)), dma((CHUNKS, 4)), dma((PARTS, 4)), dma((PARTS, 4)), dma((4,)), dma((4,)),
            ],
            compiler_params=pltpu.CompilerParams(
                collective_id=0, has_side_effects=True
            ),
            name="march",
        )(wave, lens, label, prior, attenuation, drain, diffusivity, *[jnp.asarray(f) for f in factors])
        return jnp.transpose(field, (1, 3, 0, 2)), later

    in_specs = (P(None, "harm", "tx", "ty"), P("tx", "ty"), P("tx", "ty"), P("tx", "ty"), P(), P(), P())
    out_specs = (P(None, "harm", "tx", "ty"), P("tx", "ty"))
    return jax.shard_map(body, mesh=mesh, in_specs=in_specs, out_specs=out_specs, check_vma=False)
```

```python
import math

import jax
import jax.numpy as jnp
import numpy as np
from jax import lax
from jax.experimental import pallas as pl
from jax.experimental.pallas import tpu as pltpu
from jax.sharding import PartitionSpec as P

CYCLE_READINGS = 2048
HALF = CYCLE_READINGS // 2
HARMONICS = 512
OWN = 128
ROWS = 4
COLS = 128
SEGMENTS = [(8 * i, 8) for i in range(4)] + [(16 * i, 16) for i in range(2, 8)]
ORDER = (1, 2, 0, 3, 4, 5, 6, 7, 8, 9)
CHUNKS = len(SEGMENTS)
WIDEST = 16
EARLY_PARTS = 2
PARTS = 4
PART = COLS // PARTS
PAD = 16
F32 = jnp.float32
BF16 = jnp.bfloat16

diffraction_gain = 0.3
nonlinear_gain = 0.3

TX = 16
TY = 8
AROUND = [(dy, dx) for dy in (-1, 0, 1) for dx in (-1, 0, 1) if (dy, dx) != (0, 0)]


def trig(product, period):
    angle = 2.0 * np.pi * (product % period) / period
    return np.cos(angle).astype(np.float32), np.sin(angle).astype(np.float32)


def table_factors():
    n = np.arange(1, HARMONICS + 1, dtype=np.int64)
    fine_c, fine_s = trig(n[:, None] * (2 * np.arange(128)[None, :] + 1), 2 * CYCLE_READINGS)
    coarse_c, coarse_s = trig(np.arange(8)[:, None] * np.arange(1, 17)[None, :], 16)
    coarse_c = np.repeat(coarse_c[:, :, None], 128, axis=2)
    coarse_s = np.repeat(coarse_s[:, :, None], 128, axis=2)
    far_c, far_s = trig(np.arange(64)[:, None] * n[None, :], 128)
    near_c, near_s = trig((2 * np.arange(16)[:, None] + 1) * n[None, :], 2 * CYCLE_READINGS)
    return fine_c, fine_s, coarse_c, coarse_s, far_c, far_s, near_c, near_s


def split(x):
    high = x.astype(BF16)
    return high, (x - high.astype(F32)).astype(BF16)


def product(x, high_table, low_table):
    m = x.shape[0]
    high, low = split(x)
    both = jnp.dot(jnp.concatenate([high, low], axis=0), high_table, preferred_element_type=F32)
    return both[:m] + both[m:] + jnp.dot(high, low_table, preferred_element_type=F32)


def kernel(
    wave, lens_in, label_in, prior_in, attenuation, drain, diffusivity,
    fine_c, fine_s, coarse_c, coarse_s, far_c, far_s, near_c, near_s,
    field, later,
    lens, label, prior, later_rows, raw, S, VA, VB, M, R, Y, W,
    synth_c, synth_s, anal_c, anal_s,
    factors_fine, factors_coarse, factors_far, factors_near,
    early, late, heat_rows, heat_out, wide,
    small_sem, raw_sem, load_sem, row_send, row_recv, col_send, col_recv, corner_send, corner_recv,
    early_send, early_recv, late_send, late_recv,
    one_send, one_recv, two_send, two_recv, heat_send, heat_recv,
):
    harm = lax.axis_index("harm")
    tx = lax.axis_index("tx")
    ty = lax.axis_index("ty")
    half = harm // 2
    core = harm % 2
    far_ty = (ty + 4) % TY
    wrapped = (ty + 4) // TY

    def remote(a, b, send, recv, device):
        return pltpu.make_async_remote_copy(
            src_ref=a, dst_ref=b, send_sem=send, recv_sem=recv,
            device_id=device, device_id_type=pl.DeviceIdType.MESH,
        )

    def owner(row):
        return (2 * ((row // 2 + wrapped) % 2) + row % 2, tx, far_ty)

    own_row = 2 * ((half + (far_ty + 4) // TY) % 2) + core

    def inside(dy, dx):
        ok = None
        for at, step, count in ((tx, dy, TX), (ty, dx, TY)):
            if step == 0:
                continue
            one = at > 0 if step < 0 else at < count - 1
            ok = one if ok is None else jnp.logical_and(ok, one)
        return ok

    @pl.when(tx == 0)
    def _():
        S[:, 0:4] = jnp.zeros((2, 4, COLS + 2 * PAD, OWN), F32)
        for dx in range(3):
            early[0, dx] = jnp.zeros((4, ROWS, COLS), F32)
            late[0, dx] = jnp.zeros((ROWS, COLS), F32)

    @pl.when(tx == TX - 1)
    def _():
        S[:, 8:12] = jnp.zeros((2, 4, COLS + 2 * PAD, OWN), F32)
        for dx in range(3):
            early[2, dx] = jnp.zeros((4, ROWS, COLS), F32)
            late[2, dx] = jnp.zeros((ROWS, COLS), F32)

    @pl.when(ty == 0)
    def _():
        S[:, :, 8:16] = jnp.zeros((2, 12, 8, OWN), F32)
        for dy in range(3):
            early[dy, 0] = jnp.zeros((4, ROWS, COLS), F32)

    @pl.when(ty == TY - 1)
    def _():
        S[:, :, PAD + COLS:PAD + COLS + 8] = jnp.zeros((2, 12, 8, OWN), F32)
        for dy in range(3):
            early[dy, 2] = jnp.zeros((4, ROWS, COLS), F32)

    barrier = pltpu.get_barrier_semaphore()
    for dy, dx in AROUND:
        @pl.when(inside(dy, dx))
        def _():
            pl.semaphore_signal(barrier, inc=1, device_id=(harm, tx + dy, ty + dx), device_id_type=pl.DeviceIdType.MESH)
    for dx in (-1, 0, 1):
        for j in range(4):
            pl.semaphore_signal(
                barrier, inc=1, device_id=(j, tx, (ty + dx + 4) % TY), device_id_type=pl.DeviceIdType.MESH
            )

    smalls = []
    for i, (a, b) in enumerate((
        (lens_in, lens), (label_in, label), (prior_in, prior),
    )):
        copy = pltpu.make_async_copy(a, b, small_sem.at[i])
        copy.start()
        smalls.append(copy)
    raws = []
    for p in range(2):
        for row in range(ROWS):
            copy = pltpu.make_async_copy(wave.at[p, :, row, :], raw.at[p, row], raw_sem.at[p, row])
            copy.start()
            raws.append((p, row, copy))
    loads = []
    for i, (a, b) in enumerate((
        (fine_c, factors_fine.at[0]), (fine_s, factors_fine.at[1]),
        (coarse_c, factors_coarse.at[0]), (coarse_s, factors_coarse.at[1]),
        (far_c, factors_far.at[0]), (far_s, factors_far.at[1]),
        (near_c, factors_near.at[0]), (near_s, factors_near.at[1]),
    )):
        copy = pltpu.make_async_copy(a, b, load_sem.at[i])
        copy.start()
        loads.append(copy)

    for copy in smalls:
        copy.wait()
    weight = 0.25 + 0.75 * lens[...].astype(F32)
    for p, row, copy in raws:
        copy.wait()
        S[p, 4 + row, PAD:PAD + COLS, :] = jnp.transpose(raw[p, row] * weight[row:row + 1, :])

    kinds = label[...]
    conduct = jnp.zeros((ROWS, COLS), F32)
    perfuse = jnp.zeros((ROWS, COLS), F32)
    absorb = jnp.zeros((ROWS, COLS), F32)
    for k in range(8):
        hit = kinds == k
        conduct = jnp.where(hit, diffusivity[k], conduct)
        perfuse = jnp.where(hit, drain[k], perfuse)
        absorb = jnp.where(hit, attenuation[k], absorb)
    early[1, 1, 0] = prior[...]
    early[1, 1, 1] = conduct
    early[1, 1, 2] = perfuse
    early[1, 1, 3] = absorb

    def edges(at, count):
        return jnp.where(at == 0, 1, 0) + jnp.where(at == count - 1, 1, 0)

    pl.semaphore_wait(barrier, (3 - edges(tx, TX)) * (3 - edges(ty, TY)) + 11)

    def row_copy(side, c):
        return remote(
            S.at[:, 4:8, pl.ds(PAD + SEGMENTS[c][0], SEGMENTS[c][1]), :],
            S.at[:, pl.ds(8 * side, 4), pl.ds(PAD + SEGMENTS[c][0], SEGMENTS[c][1]), :],
            row_send.at[side, c], row_recv.at[side, c], (harm, tx + 1 - 2 * side, ty),
        )

    def col_copy(side):
        return remote(
            S.at[:, 4:8, pl.ds(PAD if side else PAD + COLS - 8, 8), :],
            S.at[:, 4:8, pl.ds(PAD + COLS if side else PAD - 8, 8), :],
            col_send.at[side], col_recv.at[side], (harm, tx, ty + 1 - 2 * side),
        )

    def corner_copy(side, vertical):
        at = PAD + COLS if side else PAD - 8
        return remote(
            S.at[:, 4:8, pl.ds(at, 8), :],
            S.at[:, pl.ds(8 * vertical, 4), pl.ds(at, 8), :],
            corner_send.at[side, vertical], corner_recv.at[side, vertical],
            (harm, tx + 1 - 2 * vertical, ty),
        )

    def to_side(side):
        return tx < TX - 1 if side == 0 else tx > 0

    def from_side(side):
        return tx > 0 if side == 0 else tx < TX - 1

    def to_col(side):
        return ty < TY - 1 if side == 0 else ty > 0

    def from_col(side):
        return ty > 0 if side == 0 else ty < TY - 1

    for side in (0, 1):
        @pl.when(to_col(side))
        def _():
            col_copy(side).start()
    def start_rows(c):
        for side in (0, 1):
            @pl.when(to_side(side))
            def _():
                row_copy(side, c).start()

    for c in range(4):
        start_rows(c)

    def early_copy(dy, dx):
        slot = 3 * (dy + 1) + dx + 1
        return remote(
            early.at[1, 1], early.at[1 - dy, 1 - dx], early_send.at[slot], early_recv.at[8 - slot],
            (harm, tx + dy, ty + dx),
        )

    def late_copy(dy):
        return remote(
            late.at[1], late.at[1 - dy], late_send.at[1 + dy], late_recv.at[1 - dy], (harm, tx + dy, ty),
        )

    def late_arrival(dy):
        return remote(
            late.at[1], late.at[1 + dy], late_send.at[1 + dy], late_recv.at[1 + dy], (harm, tx + dy, ty),
        )

    for dy, dx in AROUND:
        @pl.when(inside(dy, dx))
        def _():
            early_copy(dy, dx).start()

    lane = lax.broadcasted_iota(jnp.int32, (1, OWN), 1)
    gain = diffraction_gain / (harm * OWN + lane + 1).astype(F32)

    def row_inside(row):
        at = tx * ROWS + row - 4
        return jnp.where(jnp.logical_and(at >= 0, at < TX * ROWS), 1.0, 0.0).astype(F32)

    def stencil(c):
        base, width = SEGMENTS[c]
        for k, source, target in ((1, S, VA), (2, VA, VB), (3, VB, VA), (4, VA, M)):
            low, count = (12, width) if k == 4 else (8, width + 8)
            shift = base + 4 if k == 1 else 0
            at = ty * COLS + base + low + 4 - PAD + lax.broadcasted_iota(jnp.int32, (count, OWN), 0)
            valid = jnp.logical_and(at >= 0, at < TY * COLS)
            g = jnp.where(valid, gain * (1.0 / (5 - k)), 0.0)

            def one_row(row, carry):
                gr = g * row_inside(row)
                laps = []
                for p in range(2):
                    center = source[p, row, pl.ds(shift + low, count), :]
                    laps.append(
                        source[p, row + 1, pl.ds(shift + low, count), :]
                        + source[p, row - 1, pl.ds(shift + low, count), :]
                        + source[p, row, pl.ds(shift + low + 1, count), :]
                        + source[p, row, pl.ds(shift + low - 1, count), :]
                        - 4.0 * center
                    )
                real = S[0, row, pl.ds(base + 4 + low, count), :] - gr * laps[1]
                imag = S[1, row, pl.ds(base + 4 + low, count), :] + gr * laps[0]
                if k == 4:
                    target[0, row - 4, pl.ds(base, count), :] = real
                    target[1, row - 4, pl.ds(base, count), :] = imag
                else:
                    target[0, row, pl.ds(low, count), :] = real
                    target[1, row, pl.ds(low, count), :] = imag
                return carry

            lax.fori_loop(k, 12 - k, one_row, 0)

    def one_copy(c, row):
        return remote(
            M.at[:, row, pl.ds(*SEGMENTS[c]), :],
            R.at[harm, :, pl.ds(*SEGMENTS[c]), :],
            one_send.at[c, row], one_recv.at[c, harm], owner(row),
        )

    def one_arrival(c, at, width, j):
        return remote(
            M.at[:, 0, pl.ds(at, width), :],
            R.at[j, :, pl.ds(at, width), :],
            one_send.at[c, 0], one_recv.at[c, j], (j, tx, far_ty),
        )

    def two_copy(c, j):
        return remote(
            Y.at[j, :, pl.ds(c * PART, PART), :],
            field.at[own_row, :, pl.ds(c * PART, PART), :],
            two_send.at[c, j], two_recv.at[c, own_row], (j, tx, far_ty),
        )

    def two_arrival(c, row):
        return remote(
            Y.at[0, :, pl.ds(c * PART, PART), :],
            field.at[row, :, pl.ds(c * PART, PART), :],
            two_send.at[c, 0], two_recv.at[c, row], owner(row),
        )

    def wait_rows(c):
        for side in (0, 1):
            @pl.when(from_side(side))
            def _():
                row_copy(side, c).wait_recv()

    def forward(side):
        @pl.when(from_col(side))
        def _():
            col_copy(side).wait_recv()
            for vertical in (0, 1):
                @pl.when(to_side(vertical))
                def _():
                    corner_copy(side, vertical).start()

    def wait_corners(side):
        @pl.when(from_col(side))
        def _():
            for vertical in (0, 1):
                @pl.when(from_side(vertical))
                def _():
                    corner_copy(side, vertical).wait_recv()

    def build_tables():
        for copy in loads:
            copy.wait()

        def by_time(i, carry):
            rows = pl.ds(pl.multiple_of(i * 16, 16), 16)
            fc = factors_fine[0, rows, :]
            fs = factors_fine[1, rows, :]
            for a in range(8):
                ac = factors_coarse[0, a]
                as_ = factors_coarse[1, a]
                for table, value in ((synth_c, ac * fc - as_ * fs), (synth_s, as_ * fc + ac * fs)):
                    high, low = split(value)
                    table[0, rows, a * 128:(a + 1) * 128] = high
                    table[1, rows, a * 128:(a + 1) * 128] = low
            return carry

        lax.fori_loop(0, HARMONICS // 16, by_time, 0)

        def by_harmonic(a, carry):
            rows = pl.ds(pl.multiple_of(a * 16, 16), 16)
            ac = factors_far[0, pl.ds(a, 1), :]
            as_ = factors_far[1, pl.ds(a, 1), :]
            nc = factors_near[0]
            ns = factors_near[1]
            for table, value in ((anal_c, ac * nc - as_ * ns), (anal_s, as_ * nc + ac * ns)):
                high, low = split(value)
                table[0, rows, :] = high
                table[1, rows, :] = low
            return carry

        lax.fori_loop(0, HALF // 16, by_harmonic, 0)

    forward(0)
    for c in range(4, 7):
        start_rows(c)
    forward(1)
    for c in range(7, CHUNKS):
        start_rows(c)
    arrived = 0
    for c in ORDER:
        while arrived < min(c + 2, CHUNKS):
            wait_rows(arrived)
            arrived += 1
        if c == 0:
            wait_corners(0)
        if c == CHUNKS - 1:
            wait_corners(1)
        stencil(c)
        for row in range(ROWS):
            one_copy(c, row).start()
    build_tables()

    numbers = (lax.broadcasted_iota(jnp.int32, (1, HARMONICS), 1) + 1).astype(F32)
    scale = 2.0 * math.sqrt(HARMONICS) / CYCLE_READINGS / HARMONICS
    real_factor = numbers * (nonlinear_gain / HARMONICS * 4.0 * scale)
    imag_factor = numbers * (nonlinear_gain / HARMONICS * 2.0 * scale)

    def nonlinear(c, carry):
        @pl.when(c == 0)
        def _():
            for k in range(4):
                for j in range(4):
                    one_arrival(k, 8 * k, 8, j).wait_recv()

        @pl.when(c > 0)
        def _():
            for k in range(2):
                for j in range(4):
                    one_arrival(2 + 2 * c + k, pl.multiple_of(c * PART + 16 * k, 16), 16, j).wait_recv()

        cols = pl.ds(pl.multiple_of(c * PART, PART), PART)
        real = jnp.concatenate([R[j, 0, cols, :] for j in range(4)], axis=1)
        imag = jnp.concatenate([R[j, 1, cols, :] for j in range(4)], axis=1)
        even = product(real, synth_c[0], synth_c[1])
        odd = product(imag, synth_s[0], synth_s[1])
        cosine = product(even * even + odd * odd, anal_c[0], anal_c[1])
        sine = product(even * odd, anal_s[0], anal_s[1])
        real = real - real_factor * sine
        imag = imag + imag_factor * cosine
        weighted = numbers * (real * real + imag * imag)
        W[cols, :] = weighted[:, 0:128] + weighted[:, 128:256] + weighted[:, 256:384] + weighted[:, 384:512]
        for j in range(4):
            Y[j, 0, cols, :] = real[:, 128 * j:128 * (j + 1)]
            Y[j, 1, cols, :] = imag[:, 128 * j:128 * (j + 1)]

        @pl.when(c < EARLY_PARTS)
        def _():
            for j in range(4):
                two_copy(c, j).start()

        return carry

    lax.fori_loop(0, PARTS, nonlinear, 0)

    heat_out[...] = lax.dot_general(
        jnp.ones((8, OWN), F32), W[...], (((1,), (1,)), ((), ())),
        precision=lax.Precision.HIGHEST, preferred_element_type=F32,
    )[0:1]

    def heat_copy(dx, j):
        return remote(
            heat_out, heat_rows.at[1 - dx, own_row], heat_send.at[1 + dx, j], heat_recv.at[1 - dx, own_row],
            (j, tx, (ty + dx + 4) % TY),
        )

    def heat_arrival(dx, row):
        return remote(
            heat_out, heat_rows.at[1 + dx, row], heat_send.at[1, 0], heat_recv.at[1 + dx, row],
            (row, tx, far_ty),
        )

    for dx in (-1, 0, 1):
        for j in range(4):
            heat_copy(dx, j).start()
    for c in range(EARLY_PARTS, PARTS):
        for j in range(4):
            two_copy(c, j).start()
    for dx in (-1, 0, 1):
        for row in range(ROWS):
            heat_arrival(dx, row).wait_recv()
    for dx in range(3):
        for row in range(ROWS):
            late[1, dx, row:row + 1, :] = heat_rows[dx, row]
    for dy in (-1, 1):
        @pl.when(inside(dy, 0))
        def _():
            late_copy(dy).start()
    for dy, dx in AROUND:
        @pl.when(inside(dy, dx))
        def _():
            early_copy(-dy, -dx).wait_recv()
    for dy in (-1, 1):
        @pl.when(inside(dy, 0))
        def _():
            late_arrival(dy).wait_recv()
    for dy in range(3):
        for dx in range(3):
            rows = slice(4 * dy, 4 * dy + 4)
            cols = slice(128 * dx, 128 * dx + 128)
            for k in range(4):
                wide[k, rows, cols] = early[dy, dx, k]
            wide[4, rows, cols] = late[dy, dx]
    for k in range(5):
        wide[k, 12:16, :] = jnp.zeros((4, 3 * COLS), F32)
    temperature = wide[0]
    wide_conduct = wide[1]
    wide_perfuse = wide[2]
    wide_deposit = wide[3] * wide[4] / float(HARMONICS * HARMONICS)
    for _ in range(4):
        lap = (
            pltpu.roll(temperature, 15, 0) + pltpu.roll(temperature, 1, 0)
            + pltpu.roll(temperature, 3 * COLS - 1, 1) + pltpu.roll(temperature, 1, 1)
            - 4.0 * temperature
        )
        temperature = temperature + wide_conduct * lap - wide_perfuse * temperature + wide_deposit
    wide[0] = temperature
    later_rows[...] = wide[0, 4:8, COLS:2 * COLS]
    result = pltpu.make_async_copy(later_rows, later, small_sem.at[3])
    result.start()

    for side in (0, 1):
        @pl.when(to_col(side))
        def _():
            col_copy(side).wait_send()
        for c in range(CHUNKS):
            @pl.when(to_side(side))
            def _():
                row_copy(side, c).wait_send()

        @pl.when(from_col(side))
        def _():
            for vertical in (0, 1):
                @pl.when(to_side(vertical))
                def _():
                    corner_copy(side, vertical).wait_send()
    for dy, dx in AROUND:
        @pl.when(inside(dy, dx))
        def _():
            early_copy(dy, dx).wait_send()
    for dy in (-1, 1):
        @pl.when(inside(dy, 0))
        def _():
            late_copy(dy).wait_send()
    for dx in (-1, 0, 1):
        for j in range(4):
            heat_copy(dx, j).wait_send()
    result.wait()
    for c in range(CHUNKS):
        for j in range(4):
            one_copy(c, j).wait_send()
    for c in range(PARTS):
        for j in range(4):
            two_copy(c, j).wait_send()
            two_arrival(c, j).wait_recv()


def solution(mesh):
    factors = table_factors()

    def body(wave, lens, label, prior, attenuation, drain, diffusivity):
        smem = pl.BlockSpec(memory_space=pltpu.SMEM)
        hbm = pl.BlockSpec(memory_space=pltpu.HBM)
        dma = pltpu.SemaphoreType.DMA
        field, later = pl.pallas_call(
            kernel,
            out_shape=(
                jax.ShapeDtypeStruct((ROWS, 2, COLS, OWN), F32),
                jax.ShapeDtypeStruct((ROWS, COLS), F32),
            ),
            in_specs=[hbm] * 4 + [smem] * 3 + [hbm] * 8,
            out_specs=(hbm, hbm),
            scratch_shapes=[
                pltpu.VMEM((ROWS, COLS), jnp.int32), pltpu.VMEM((ROWS, COLS), jnp.int32), pltpu.VMEM((ROWS, COLS), F32),
                pltpu.VMEM((ROWS, COLS), F32),
                pltpu.VMEM((2, ROWS, OWN, COLS), F32),
                pltpu.VMEM((2, 12, COLS + 2 * PAD, OWN), F32),
                pltpu.VMEM((2, 12, WIDEST + 2 * PAD, OWN), F32),
                pltpu.VMEM((2, 12, WIDEST + 2 * PAD, OWN), F32),
                pltpu.VMEM((2, ROWS, COLS, OWN), F32),
                pltpu.VMEM((4, 2, COLS, OWN), F32),
                pltpu.VMEM((4, 2, COLS, OWN), F32),
                pltpu.VMEM((COLS, OWN), F32),
                pltpu.VMEM((2, HARMONICS, HALF), BF16),
                pltpu.VMEM((2, HARMONICS, HALF), BF16),
                pltpu.VMEM((2, HALF, HARMONICS), BF16),
                pltpu.VMEM((2, HALF, HARMONICS), BF16),
                pltpu.VMEM((2, HARMONICS, 128), F32),
                pltpu.VMEM((2, 8, 16, 128), F32),
                pltpu.VMEM((2, 64, HARMONICS), F32),
                pltpu.VMEM((2, 16, HARMONICS), F32),
                pltpu.VMEM((3, 3, 4, ROWS, COLS), F32),
                pltpu.VMEM((3, 3, ROWS, COLS), F32),
                pltpu.VMEM((3, ROWS, 1, COLS), F32),
                pltpu.VMEM((1, COLS), F32),
                pltpu.VMEM((5, 16, 3 * COLS), F32),
                dma((4,)), dma((2, ROWS)), dma((8,)), dma((2, CHUNKS)), dma((2, CHUNKS)), dma((2,)), dma((2,)), dma((2, 2)), dma((2, 2)),
                dma((9,)), dma((9,)), dma((3,)), dma((3,)),
                dma((CHUNKS, 4)), dma((CHUNKS, 4)), dma((PARTS, 4)), dma((PARTS, 4)), dma((3, 4)), dma((3, 4)),
            ],
            compiler_params=pltpu.CompilerParams(
                collective_id=0, has_side_effects=True
            ),
            name="march",
        )(wave, lens, label, prior, attenuation, drain, diffusivity, *[jnp.asarray(f) for f in factors])
        return jnp.transpose(field, (1, 3, 0, 2)), later

    in_specs = (P(None, "harm", "tx", "ty"), P("tx", "ty"), P("tx", "ty"), P("tx", "ty"), P(), P(), P())
    out_specs = (P(None, "harm", "tx", "ty"), P("tx", "ty"))
    return jax.shard_map(body, mesh=mesh, in_specs=in_specs, out_specs=out_specs, check_vma=False)
```

```python
import math

import jax
import jax.numpy as jnp
import numpy as np
from jax import lax
from jax.experimental import pallas as pl
from jax.experimental.pallas import tpu as pltpu
from jax.sharding import PartitionSpec as P

CYCLE_READINGS = 2048
HALF = CYCLE_READINGS // 2
HARMONICS = 512
OWN = 128
ROWS = 4
COLS = 128
SEGMENTS = [(8 * i, 8) for i in range(4)] + [(16 * i, 16) for i in range(2, 8)]
ORDER = (1, 2, 0, 3, 4, 5, 6, 7, 8, 9)
CHUNKS = len(SEGMENTS)
WIDEST = 16
EARLY_PARTS = 2
PARTS = 4
PART = COLS // PARTS
PAD = 16
F32 = jnp.float32
BF16 = jnp.bfloat16

diffraction_gain = 0.3
nonlinear_gain = 0.3

TX = 16
TY = 8
AROUND = [(dy, dx) for dy in (-1, 0, 1) for dx in (-1, 0, 1) if (dy, dx) != (0, 0)]


def trig(product, period):
    angle = 2.0 * np.pi * (product % period) / period
    return np.cos(angle).astype(np.float32), np.sin(angle).astype(np.float32)


def table_factors():
    n = np.arange(1, HARMONICS + 1, dtype=np.int64)
    fine_c, fine_s = trig(n[:, None] * (2 * np.arange(128)[None, :] + 1), 2 * CYCLE_READINGS)
    coarse_c, coarse_s = trig(np.arange(8)[:, None] * np.arange(1, 17)[None, :], 16)
    coarse_c = np.repeat(coarse_c[:, :, None], 128, axis=2)
    coarse_s = np.repeat(coarse_s[:, :, None], 128, axis=2)
    far_c, far_s = trig(np.arange(64)[:, None] * n[None, :], 128)
    near_c, near_s = trig((2 * np.arange(16)[:, None] + 1) * n[None, :], 2 * CYCLE_READINGS)
    return fine_c, fine_s, coarse_c, coarse_s, far_c, far_s, near_c, near_s


def split(x):
    high = x.astype(BF16)
    return high, (x - high.astype(F32)).astype(BF16)


def product(x, high_table, low_table):
    m = x.shape[0]
    high, low = split(x)
    both = jnp.dot(jnp.concatenate([high, low], axis=0), high_table, preferred_element_type=F32)
    return both[:m] + both[m:] + jnp.dot(high, low_table, preferred_element_type=F32)


def kernel(
    wave, lens_in, label_in, prior_in, attenuation_in, drain_in, diffusivity_in,
    fine_c, fine_s, coarse_c, coarse_s, far_c, far_s, near_c, near_s,
    field, later,
    lens, label, prior, attenuation, drain, diffusivity, raw, S, VA, VB, M, R, Y, W,
    synth_c, synth_s, anal_c, anal_s,
    factors_fine, factors_coarse, factors_far, factors_near,
    early, late, heat_rows, heat_out, wide,
    small_sem, raw_sem, load_sem, row_send, row_recv, col_send, col_recv, corner_send, corner_recv,
    early_send, early_recv, late_send, late_recv,
    one_send, one_recv, two_send, two_recv, heat_send, heat_recv,
):
    harm = lax.axis_index("harm")
    tx = lax.axis_index("tx")
    ty = lax.axis_index("ty")
    half = harm // 2
    core = harm % 2
    far_ty = (ty + 4) % TY
    wrapped = (ty + 4) // TY

    def remote(a, b, send, recv, device):
        return pltpu.make_async_remote_copy(
            src_ref=a, dst_ref=b, send_sem=send, recv_sem=recv,
            device_id=device, device_id_type=pl.DeviceIdType.MESH,
        )

    def owner(row):
        return (2 * ((row // 2 + wrapped) % 2) + row % 2, tx, far_ty)

    own_row = 2 * ((half + (far_ty + 4) // TY) % 2) + core

    def inside(dy, dx):
        ok = None
        for at, step, count in ((tx, dy, TX), (ty, dx, TY)):
            if step == 0:
                continue
            one = at > 0 if step < 0 else at < count - 1
            ok = one if ok is None else jnp.logical_and(ok, one)
        return ok

    @pl.when(tx == 0)
    def _():
        S[:, 0:4] = jnp.zeros((2, 4, COLS + 2 * PAD, OWN), F32)
        for dx in range(3):
            early[0, dx] = jnp.zeros((4, ROWS, COLS), F32)
            late[0, dx] = jnp.zeros((ROWS, COLS), F32)

    @pl.when(tx == TX - 1)
    def _():
        S[:, 8:12] = jnp.zeros((2, 4, COLS + 2 * PAD, OWN), F32)
        for dx in range(3):
            early[2, dx] = jnp.zeros((4, ROWS, COLS), F32)
            late[2, dx] = jnp.zeros((ROWS, COLS), F32)

    @pl.when(ty == 0)
    def _():
        S[:, :, 8:16] = jnp.zeros((2, 12, 8, OWN), F32)
        for dy in range(3):
            early[dy, 0] = jnp.zeros((4, ROWS, COLS), F32)

    @pl.when(ty == TY - 1)
    def _():
        S[:, :, PAD + COLS:PAD + COLS + 8] = jnp.zeros((2, 12, 8, OWN), F32)
        for dy in range(3):
            early[dy, 2] = jnp.zeros((4, ROWS, COLS), F32)

    barrier = pltpu.get_barrier_semaphore()
    for dy, dx in AROUND:
        @pl.when(inside(dy, dx))
        def _():
            pl.semaphore_signal(barrier, inc=1, device_id=(harm, tx + dy, ty + dx), device_id_type=pl.DeviceIdType.MESH)
    for dx in (-1, 0, 1):
        for j in range(4):
            pl.semaphore_signal(
                barrier, inc=1, device_id=(j, tx, (ty + dx + 4) % TY), device_id_type=pl.DeviceIdType.MESH
            )

    smalls = []
    for i, (a, b) in enumerate((
        (lens_in, lens), (label_in, label), (prior_in, prior),
        (attenuation_in, attenuation), (drain_in, drain), (diffusivity_in, diffusivity),
    )):
        copy = pltpu.make_async_copy(a, b, small_sem.at[i])
        copy.start()
        smalls.append(copy)
    raws = []
    for p in range(2):
        for row in range(ROWS):
            copy = pltpu.make_async_copy(wave.at[p, :, row, :], raw.at[p, row], raw_sem.at[p, row])
            copy.start()
            raws.append((p, row, copy))
    loads = []
    for i, (a, b) in enumerate((
        (fine_c, factors_fine.at[0]), (fine_s, factors_fine.at[1]),
        (coarse_c, factors_coarse.at[0]), (coarse_s, factors_coarse.at[1]),
        (far_c, factors_far.at[0]), (far_s, factors_far.at[1]),
        (near_c, factors_near.at[0]), (near_s, factors_near.at[1]),
    )):
        copy = pltpu.make_async_copy(a, b, load_sem.at[i])
        copy.start()
        loads.append(copy)

    for copy in smalls:
        copy.wait()
    weight = 0.25 + 0.75 * lens[...].astype(F32)
    for p, row, copy in raws:
        copy.wait()
        S[p, 4 + row, PAD:PAD + COLS, :] = jnp.transpose(raw[p, row] * weight[row:row + 1, :])

    kinds = label[...]
    conduct = jnp.zeros((ROWS, COLS), F32)
    perfuse = jnp.zeros((ROWS, COLS), F32)
    absorb = jnp.zeros((ROWS, COLS), F32)
    for k in range(8):
        hit = kinds == k
        conduct = jnp.where(hit, diffusivity[k], conduct)
        perfuse = jnp.where(hit, drain[k], perfuse)
        absorb = jnp.where(hit, attenuation[k], absorb)
    early[1, 1, 0] = prior[...]
    early[1, 1, 1] = conduct
    early[1, 1, 2] = perfuse
    early[1, 1, 3] = absorb

    def edges(at, count):
        return jnp.where(at == 0, 1, 0) + jnp.where(at == count - 1, 1, 0)

    pl.semaphore_wait(barrier, (3 - edges(tx, TX)) * (3 - edges(ty, TY)) + 11)

    def row_copy(side, c):
        return remote(
            S.at[:, 4:8, pl.ds(PAD + SEGMENTS[c][0], SEGMENTS[c][1]), :],
            S.at[:, pl.ds(8 * side, 4), pl.ds(PAD + SEGMENTS[c][0], SEGMENTS[c][1]), :],
            row_send.at[side, c], row_recv.at[side, c], (harm, tx + 1 - 2 * side, ty),
        )

    def col_copy(side):
        return remote(
            S.at[:, 4:8, pl.ds(PAD if side else PAD + COLS - 8, 8), :],
            S.at[:, 4:8, pl.ds(PAD + COLS if side else PAD - 8, 8), :],
            col_send.at[side], col_recv.at[side], (harm, tx, ty + 1 - 2 * side),
        )

    def corner_copy(side, vertical):
        at = PAD + COLS if side else PAD - 8
        return remote(
            S.at[:, 4:8, pl.ds(at, 8), :],
            S.at[:, pl.ds(8 * vertical, 4), pl.ds(at, 8), :],
            corner_send.at[side, vertical], corner_recv.at[side, vertical],
            (harm, tx + 1 - 2 * vertical, ty),
        )

    def to_side(side):
        return tx < TX - 1 if side == 0 else tx > 0

    def from_side(side):
        return tx > 0 if side == 0 else tx < TX - 1

    def to_col(side):
        return ty < TY - 1 if side == 0 else ty > 0

    def from_col(side):
        return ty > 0 if side == 0 else ty < TY - 1

    for side in (0, 1):
        @pl.when(to_col(side))
        def _():
            col_copy(side).start()
    def start_rows(c):
        for side in (0, 1):
            @pl.when(to_side(side))
            def _():
                row_copy(side, c).start()

    for c in range(4):
        start_rows(c)

    def early_copy(dy, dx):
        slot = 3 * (dy + 1) + dx + 1
        return remote(
            early.at[1, 1], early.at[1 - dy, 1 - dx], early_send.at[slot], early_recv.at[8 - slot],
            (harm, tx + dy, ty + dx),
        )

    def late_copy(dy):
        return remote(
            late.at[1], late.at[1 - dy], late_send.at[1 + dy], late_recv.at[1 - dy], (harm, tx + dy, ty),
        )

    def late_arrival(dy):
        return remote(
            late.at[1], late.at[1 + dy], late_send.at[1 + dy], late_recv.at[1 + dy], (harm, tx + dy, ty),
        )

    for dy, dx in AROUND:
        @pl.when(inside(dy, dx))
        def _():
            early_copy(dy, dx).start()

    lane = lax.broadcasted_iota(jnp.int32, (1, OWN), 1)
    gain = diffraction_gain / (harm * OWN + lane + 1).astype(F32)

    def row_inside(row):
        at = tx * ROWS + row - 4
        return jnp.where(jnp.logical_and(at >= 0, at < TX * ROWS), 1.0, 0.0).astype(F32)

    def stencil(c):
        base, width = SEGMENTS[c]
        for k, source, target in ((1, S, VA), (2, VA, VB), (3, VB, VA), (4, VA, M)):
            low, count = (12, width) if k == 4 else (8, width + 8)
            shift = base + 4 if k == 1 else 0
            at = ty * COLS + base + low + 4 - PAD + lax.broadcasted_iota(jnp.int32, (count, OWN), 0)
            valid = jnp.logical_and(at >= 0, at < TY * COLS)
            g = jnp.where(valid, gain * (1.0 / (5 - k)), 0.0)

            def one_row(row, carry):
                gr = g * row_inside(row)
                laps = []
                for p in range(2):
                    center = source[p, row, pl.ds(shift + low, count), :]
                    laps.append(
                        source[p, row + 1, pl.ds(shift + low, count), :]
                        + source[p, row - 1, pl.ds(shift + low, count), :]
                        + source[p, row, pl.ds(shift + low + 1, count), :]
                        + source[p, row, pl.ds(shift + low - 1, count), :]
                        - 4.0 * center
                    )
                real = S[0, row, pl.ds(base + 4 + low, count), :] - gr * laps[1]
                imag = S[1, row, pl.ds(base + 4 + low, count), :] + gr * laps[0]
                if k == 4:
                    target[0, row - 4, pl.ds(base, count), :] = real
                    target[1, row - 4, pl.ds(base, count), :] = imag
                else:
                    target[0, row, pl.ds(low, count), :] = real
                    target[1, row, pl.ds(low, count), :] = imag
                return carry

            lax.fori_loop(k, 12 - k, one_row, 0)

    def one_copy(c, row):
        return remote(
            M.at[:, row, pl.ds(*SEGMENTS[c]), :],
            R.at[harm, :, pl.ds(*SEGMENTS[c]), :],
            one_send.at[c, row], one_recv.at[c, harm], owner(row),
        )

    def one_arrival(c, at, width, j):
        return remote(
            M.at[:, 0, pl.ds(at, width), :],
            R.at[j, :, pl.ds(at, width), :],
            one_send.at[c, 0], one_recv.at[c, j], (j, tx, far_ty),
        )

    def two_copy(c, j):
        return remote(
            Y.at[j, :, pl.ds(c * PART, PART), :],
            field.at[own_row, :, pl.ds(c * PART, PART), :],
            two_send.at[c, j], two_recv.at[c, own_row], (j, tx, far_ty),
        )

    def two_arrival(c, row):
        return remote(
            Y.at[0, :, pl.ds(c * PART, PART), :],
            field.at[row, :, pl.ds(c * PART, PART), :],
            two_send.at[c, 0], two_recv.at[c, row], owner(row),
        )

    def wait_rows(c):
        for side in (0, 1):
            @pl.when(from_side(side))
            def _():
                row_copy(side, c).wait_recv()

    def forward(side):
        @pl.when(from_col(side))
        def _():
            col_copy(side).wait_recv()
            for vertical in (0, 1):
                @pl.when(to_side(vertical))
                def _():
                    corner_copy(side, vertical).start()

    def wait_corners(side):
        @pl.when(from_col(side))
        def _():
            for vertical in (0, 1):
                @pl.when(from_side(vertical))
                def _():
                    corner_copy(side, vertical).wait_recv()

    def build_tables():
        for copy in loads:
            copy.wait()

        def by_time(i, carry):
            rows = pl.ds(pl.multiple_of(i * 16, 16), 16)
            fc = factors_fine[0, rows, :]
            fs = factors_fine[1, rows, :]
            for a in range(8):
                ac = factors_coarse[0, a]
                as_ = factors_coarse[1, a]
                for table, value in ((synth_c, ac * fc - as_ * fs), (synth_s, as_ * fc + ac * fs)):
                    high, low = split(value)
                    table[0, rows, a * 128:(a + 1) * 128] = high
                    table[1, rows, a * 128:(a + 1) * 128] = low
            return carry

        lax.fori_loop(0, HARMONICS // 16, by_time, 0)

        def by_harmonic(a, carry):
            rows = pl.ds(pl.multiple_of(a * 16, 16), 16)
            ac = factors_far[0, pl.ds(a, 1), :]
            as_ = factors_far[1, pl.ds(a, 1), :]
            nc = factors_near[0]
            ns = factors_near[1]
            for table, value in ((anal_c, ac * nc - as_ * ns), (anal_s, as_ * nc + ac * ns)):
                high, low = split(value)
                table[0, rows, :] = high
                table[1, rows, :] = low
            return carry

        lax.fori_loop(0, HALF // 16, by_harmonic, 0)

    forward(0)
    for c in range(4, 7):
        start_rows(c)
    forward(1)
    for c in range(7, CHUNKS):
        start_rows(c)
    arrived = 0
    for c in ORDER:
        while arrived < min(c + 2, CHUNKS):
            wait_rows(arrived)
            arrived += 1
        if c == 0:
            wait_corners(0)
        if c == CHUNKS - 1:
            wait_corners(1)
        stencil(c)
        for row in range(ROWS):
            one_copy(c, row).start()
    build_tables()

    numbers = (lax.broadcasted_iota(jnp.int32, (1, HARMONICS), 1) + 1).astype(F32)
    scale = 2.0 * math.sqrt(HARMONICS) / CYCLE_READINGS / HARMONICS
    real_factor = numbers * (nonlinear_gain / HARMONICS * 4.0 * scale)
    imag_factor = numbers * (nonlinear_gain / HARMONICS * 2.0 * scale)

    def nonlinear(c, carry):
        @pl.when(c == 0)
        def _():
            for k in range(4):
                for j in range(4):
                    one_arrival(k, 8 * k, 8, j).wait_recv()

        @pl.when(c > 0)
        def _():
            for k in range(2):
                for j in range(4):
                    one_arrival(2 + 2 * c + k, pl.multiple_of(c * PART + 16 * k, 16), 16, j).wait_recv()

        cols = pl.ds(pl.multiple_of(c * PART, PART), PART)
        real = jnp.concatenate([R[j, 0, cols, :] for j in range(4)], axis=1)
        imag = jnp.concatenate([R[j, 1, cols, :] for j in range(4)], axis=1)
        even = product(real, synth_c[0], synth_c[1])
        odd = product(imag, synth_s[0], synth_s[1])
        cosine = product(even * even + odd * odd, anal_c[0], anal_c[1])
        sine = product(even * odd, anal_s[0], anal_s[1])
        real = real - real_factor * sine
        imag = imag + imag_factor * cosine
        weighted = numbers * (real * real + imag * imag)
        W[cols, :] = weighted[:, 0:128] + weighted[:, 128:256] + weighted[:, 256:384] + weighted[:, 384:512]
        for j in range(4):
            Y[j, 0, cols, :] = real[:, 128 * j:128 * (j + 1)]
            Y[j, 1, cols, :] = imag[:, 128 * j:128 * (j + 1)]

        @pl.when(c < EARLY_PARTS)
        def _():
            for j in range(4):
                two_copy(c, j).start()

        return carry

    lax.fori_loop(0, PARTS, nonlinear, 0)

    heat_out[...] = lax.dot_general(
        jnp.ones((8, OWN), F32), W[...], (((1,), (1,)), ((), ())),
        precision=lax.Precision.HIGHEST, preferred_element_type=F32,
    )[0:1]

    def heat_copy(dx, j):
        return remote(
            heat_out, heat_rows.at[1 - dx, own_row], heat_send.at[1 + dx, j], heat_recv.at[1 - dx, own_row],
            (j, tx, (ty + dx + 4) % TY),
        )

    def heat_arrival(dx, row):
        return remote(
            heat_out, heat_rows.at[1 + dx, row], heat_send.at[1, 0], heat_recv.at[1 + dx, row],
            (row, tx, far_ty),
        )

    for dx in (-1, 0, 1):
        for j in range(4):
            heat_copy(dx, j).start()
    for c in range(EARLY_PARTS, PARTS):
        for j in range(4):
            two_copy(c, j).start()
    for dx in (-1, 0, 1):
        for row in range(ROWS):
            heat_arrival(dx, row).wait_recv()
    for dx in range(3):
        for row in range(ROWS):
            late[1, dx, row:row + 1, :] = heat_rows[dx, row]
    for dy in (-1, 1):
        @pl.when(inside(dy, 0))
        def _():
            late_copy(dy).start()
    for dy, dx in AROUND:
        @pl.when(inside(dy, dx))
        def _():
            early_copy(-dy, -dx).wait_recv()
    for dy in (-1, 1):
        @pl.when(inside(dy, 0))
        def _():
            late_arrival(dy).wait_recv()
    for dy in range(3):
        for dx in range(3):
            rows = slice(4 * dy, 4 * dy + 4)
            cols = slice(128 * dx, 128 * dx + 128)
            for k in range(4):
                wide[k, rows, cols] = early[dy, dx, k]
            wide[4, rows, cols] = late[dy, dx]
    for k in range(5):
        wide[k, 12:16, :] = jnp.zeros((4, 3 * COLS), F32)
    temperature = wide[0]
    wide_conduct = wide[1]
    wide_perfuse = wide[2]
    wide_deposit = wide[3] * wide[4] / float(HARMONICS * HARMONICS)
    for _ in range(4):
        lap = (
            pltpu.roll(temperature, 15, 0) + pltpu.roll(temperature, 1, 0)
            + pltpu.roll(temperature, 3 * COLS - 1, 1) + pltpu.roll(temperature, 1, 1)
            - 4.0 * temperature
        )
        temperature = temperature + wide_conduct * lap - wide_perfuse * temperature + wide_deposit
    wide[0] = temperature
    later[...] = wide[0, 4:8, COLS:2 * COLS]

    for side in (0, 1):
        @pl.when(to_col(side))
        def _():
            col_copy(side).wait_send()
        for c in range(CHUNKS):
            @pl.when(to_side(side))
            def _():
                row_copy(side, c).wait_send()

        @pl.when(from_col(side))
        def _():
            for vertical in (0, 1):
                @pl.when(to_side(vertical))
                def _():
                    corner_copy(side, vertical).wait_send()
    for dy, dx in AROUND:
        @pl.when(inside(dy, dx))
        def _():
            early_copy(dy, dx).wait_send()
    for dy in (-1, 1):
        @pl.when(inside(dy, 0))
        def _():
            late_copy(dy).wait_send()
    for dx in (-1, 0, 1):
        for j in range(4):
            heat_copy(dx, j).wait_send()
    for c in range(CHUNKS):
        for j in range(4):
            one_copy(c, j).wait_send()
    for c in range(PARTS):
        for j in range(4):
            two_copy(c, j).wait_send()
            two_arrival(c, j).wait_recv()


def solution(mesh):
    factors = table_factors()

    def body(wave, lens, label, prior, attenuation, drain, diffusivity):
        vmem = pl.BlockSpec(memory_space=pltpu.VMEM)
        anywhere = pl.BlockSpec(memory_space=pl.ANY)
        def in_hbm(x):
            return pltpu.with_memory_space_constraint(x, pltpu.HBM)

        hbm = pl.BlockSpec(memory_space=pltpu.HBM)
        dma = pltpu.SemaphoreType.DMA
        field, later = pl.pallas_call(
            kernel,
            out_shape=(
                jax.ShapeDtypeStruct((ROWS, 2, COLS, OWN), F32),
                jax.ShapeDtypeStruct((ROWS, COLS), F32),
            ),
            in_specs=[hbm] * 15,
            out_specs=(anywhere, vmem),
            scratch_shapes=[
                pltpu.VMEM((ROWS, COLS), jnp.int32), pltpu.VMEM((ROWS, COLS), jnp.int32), pltpu.VMEM((ROWS, COLS), F32),
                pltpu.SMEM((8,), F32), pltpu.SMEM((8,), F32), pltpu.SMEM((8,), F32),
                pltpu.VMEM((2, ROWS, OWN, COLS), F32),
                pltpu.VMEM((2, 12, COLS + 2 * PAD, OWN), F32),
                pltpu.VMEM((2, 12, WIDEST + 2 * PAD, OWN), F32),
                pltpu.VMEM((2, 12, WIDEST + 2 * PAD, OWN), F32),
                pltpu.VMEM((2, ROWS, COLS, OWN), F32),
                pltpu.VMEM((4, 2, COLS, OWN), F32),
                pltpu.VMEM((4, 2, COLS, OWN), F32),
                pltpu.VMEM((COLS, OWN), F32),
                pltpu.VMEM((2, HARMONICS, HALF), BF16),
                pltpu.VMEM((2, HARMONICS, HALF), BF16),
                pltpu.VMEM((2, HALF, HARMONICS), BF16),
                pltpu.VMEM((2, HALF, HARMONICS), BF16),
                pltpu.VMEM((2, HARMONICS, 128), F32),
                pltpu.VMEM((2, 8, 16, 128), F32),
                pltpu.VMEM((2, 64, HARMONICS), F32),
                pltpu.VMEM((2, 16, HARMONICS), F32),
                pltpu.VMEM((3, 3, 4, ROWS, COLS), F32),
                pltpu.VMEM((3, 3, ROWS, COLS), F32),
                pltpu.VMEM((3, ROWS, 1, COLS), F32),
                pltpu.VMEM((1, COLS), F32),
                pltpu.VMEM((5, 16, 3 * COLS), F32),
                dma((6,)), dma((2, ROWS)), dma((8,)), dma((2, CHUNKS)), dma((2, CHUNKS)), dma((2,)), dma((2,)), dma((2, 2)), dma((2, 2)),
                dma((9,)), dma((9,)), dma((3,)), dma((3,)),
                dma((CHUNKS, 4)), dma((CHUNKS, 4)), dma((PARTS, 4)), dma((PARTS, 4)), dma((3, 4)), dma((3, 4)),
            ],
            compiler_params=pltpu.CompilerParams(
                collective_id=0, has_side_effects=True, vmem_limit_bytes=48 << 20
            ),
            name="march",
        )(*[in_hbm(a) for a in (wave, lens, label, prior, attenuation, drain, diffusivity)], *[in_hbm(jnp.asarray(f)) for f in factors])
        return jnp.transpose(field, (1, 3, 0, 2)), later

    in_specs = (P(None, "harm", "tx", "ty"), P("tx", "ty"), P("tx", "ty"), P("tx", "ty"), P(), P(), P())
    out_specs = (P(None, "harm", "tx", "ty"), P("tx", "ty"))
    return jax.shard_map(body, mesh=mesh, in_specs=in_specs, out_specs=out_specs, check_vma=False)
```

```python
import math

import jax
import jax.numpy as jnp
import numpy as np
from jax import lax
from jax.experimental import pallas as pl
from jax.experimental.pallas import tpu as pltpu
from jax.sharding import PartitionSpec as P

CYCLE_READINGS = 2048
HALF = CYCLE_READINGS // 2
HARMONICS = 512
OWN = 128
ROWS = 4
COLS = 128
SEGMENTS = [(8 * i, 8) for i in range(4)] + [(16 * i, 16) for i in range(2, 8)]
ORDER = (1, 2, 0, 3, 4, 5, 6, 7, 8, 9)
CHUNKS = len(SEGMENTS)
WIDEST = 16
EARLY_PARTS = 1
PARTS = 4
PART = COLS // PARTS
PAD = 16
F32 = jnp.float32
BF16 = jnp.bfloat16

diffraction_gain = 0.3
nonlinear_gain = 0.3

TX = 16
TY = 8
AROUND = [(dy, dx) for dy in (-1, 0, 1) for dx in (-1, 0, 1) if (dy, dx) != (0, 0)]


def trig(product, period):
    angle = 2.0 * np.pi * (product % period) / period
    return np.cos(angle).astype(np.float32), np.sin(angle).astype(np.float32)


def table_factors():
    n = np.arange(1, HARMONICS + 1, dtype=np.int64)
    fine_c, fine_s = trig(n[:, None] * (2 * np.arange(128)[None, :] + 1), 2 * CYCLE_READINGS)
    coarse_c, coarse_s = trig(np.arange(8)[:, None] * np.arange(1, 17)[None, :], 16)
    coarse_c = np.repeat(coarse_c[:, :, None], 128, axis=2)
    coarse_s = np.repeat(coarse_s[:, :, None], 128, axis=2)
    far_c, far_s = trig(np.arange(64)[:, None] * n[None, :], 128)
    near_c, near_s = trig((2 * np.arange(16)[:, None] + 1) * n[None, :], 2 * CYCLE_READINGS)
    return fine_c, fine_s, coarse_c, coarse_s, far_c, far_s, near_c, near_s


def split(x):
    high = x.astype(BF16)
    return high, (x - high.astype(F32)).astype(BF16)


def product(x, high_table, low_table):
    m = x.shape[0]
    high, low = split(x)
    both = jnp.dot(jnp.concatenate([high, low], axis=0), high_table, preferred_element_type=F32)
    return both[:m] + both[m:] + jnp.dot(high, low_table, preferred_element_type=F32)


def kernel(
    wave, lens_in, label_in, prior_in, attenuation_in, drain_in, diffusivity_in,
    fine_c, fine_s, coarse_c, coarse_s, far_c, far_s, near_c, near_s,
    field, later,
    lens, label, prior, attenuation, drain, diffusivity, raw, S, VA, VB, M, R, Y, W,
    synth_c, synth_s, anal_c, anal_s,
    factors_fine, factors_coarse, factors_far, factors_near,
    early, late, heat_rows, heat_out, wide,
    small_sem, raw_sem, load_sem, row_send, row_recv, col_send, col_recv, corner_send, corner_recv,
    early_send, early_recv, late_send, late_recv,
    one_send, one_recv, two_send, two_recv, heat_send, heat_recv,
):
    harm = lax.axis_index("harm")
    tx = lax.axis_index("tx")
    ty = lax.axis_index("ty")
    half = harm // 2
    core = harm % 2
    far_ty = (ty + 4) % TY
    wrapped = (ty + 4) // TY

    def remote(a, b, send, recv, device):
        return pltpu.make_async_remote_copy(
            src_ref=a, dst_ref=b, send_sem=send, recv_sem=recv,
            device_id=device, device_id_type=pl.DeviceIdType.MESH,
        )

    def owner(row):
        return (2 * ((row // 2 + wrapped) % 2) + row % 2, tx, far_ty)

    own_row = 2 * ((half + (far_ty + 4) // TY) % 2) + core

    def inside(dy, dx):
        ok = None
        for at, step, count in ((tx, dy, TX), (ty, dx, TY)):
            if step == 0:
                continue
            one = at > 0 if step < 0 else at < count - 1
            ok = one if ok is None else jnp.logical_and(ok, one)
        return ok

    @pl.when(tx == 0)
    def _():
        S[:, 0:4] = jnp.zeros((2, 4, COLS + 2 * PAD, OWN), F32)
        for dx in range(3):
            early[0, dx] = jnp.zeros((4, ROWS, COLS), F32)
            late[0, dx] = jnp.zeros((ROWS, COLS), F32)

    @pl.when(tx == TX - 1)
    def _():
        S[:, 8:12] = jnp.zeros((2, 4, COLS + 2 * PAD, OWN), F32)
        for dx in range(3):
            early[2, dx] = jnp.zeros((4, ROWS, COLS), F32)
            late[2, dx] = jnp.zeros((ROWS, COLS), F32)

    @pl.when(ty == 0)
    def _():
        S[:, :, 8:16] = jnp.zeros((2, 12, 8, OWN), F32)
        for dy in range(3):
            early[dy, 0] = jnp.zeros((4, ROWS, COLS), F32)
        for row in range(ROWS):
            heat_rows[0, row] = jnp.zeros((1, COLS), F32)

    @pl.when(ty == TY - 1)
    def _():
        S[:, :, PAD + COLS:PAD + COLS + 8] = jnp.zeros((2, 12, 8, OWN), F32)
        for dy in range(3):
            early[dy, 2] = jnp.zeros((4, ROWS, COLS), F32)
        for row in range(ROWS):
            heat_rows[2, row] = jnp.zeros((1, COLS), F32)

    barrier = pltpu.get_barrier_semaphore()
    for dy, dx in AROUND:
        @pl.when(inside(dy, dx))
        def _():
            pl.semaphore_signal(barrier, inc=1, device_id=(harm, tx + dy, ty + dx), device_id_type=pl.DeviceIdType.MESH)
    for j in range(4):
        pl.semaphore_signal(barrier, inc=1, device_id=(j, tx, far_ty), device_id_type=pl.DeviceIdType.MESH)

    smalls = []
    for i, (a, b) in enumerate((
        (lens_in, lens), (label_in, label), (prior_in, prior),
        (attenuation_in, attenuation), (drain_in, drain), (diffusivity_in, diffusivity),
    )):
        copy = pltpu.make_async_copy(a, b, small_sem.at[i])
        copy.start()
        smalls.append(copy)
    raws = []
    for p in range(2):
        for row in range(ROWS):
            copy = pltpu.make_async_copy(wave.at[p, :, row, :], raw.at[p, row], raw_sem.at[p, row])
            copy.start()
            raws.append((p, row, copy))
    loads = []
    for i, (a, b) in enumerate((
        (fine_c, factors_fine.at[0]), (fine_s, factors_fine.at[1]),
        (coarse_c, factors_coarse.at[0]), (coarse_s, factors_coarse.at[1]),
        (far_c, factors_far.at[0]), (far_s, factors_far.at[1]),
        (near_c, factors_near.at[0]), (near_s, factors_near.at[1]),
    )):
        copy = pltpu.make_async_copy(a, b, load_sem.at[i])
        copy.start()
        loads.append(copy)

    for copy in smalls:
        copy.wait()
    weight = 0.25 + 0.75 * lens[...].astype(F32)
    for p, row, copy in raws:
        copy.wait()
        S[p, 4 + row, PAD:PAD + COLS, :] = jnp.transpose(raw[p, row] * weight[row:row + 1, :])

    kinds = label[...]
    conduct = jnp.zeros((ROWS, COLS), F32)
    perfuse = jnp.zeros((ROWS, COLS), F32)
    absorb = jnp.zeros((ROWS, COLS), F32)
    for k in range(8):
        hit = kinds == k
        conduct = jnp.where(hit, diffusivity[k], conduct)
        perfuse = jnp.where(hit, drain[k], perfuse)
        absorb = jnp.where(hit, attenuation[k], absorb)
    early[1, 1, 0] = prior[...]
    early[1, 1, 1] = conduct
    early[1, 1, 2] = perfuse
    early[1, 1, 3] = absorb

    def edges(at, count):
        return jnp.where(at == 0, 1, 0) + jnp.where(at == count - 1, 1, 0)

    pl.semaphore_wait(barrier, (3 - edges(tx, TX)) * (3 - edges(ty, TY)) + 3)

    def row_copy(side, c):
        return remote(
            S.at[:, 4:8, pl.ds(PAD + SEGMENTS[c][0], SEGMENTS[c][1]), :],
            S.at[:, pl.ds(8 * side, 4), pl.ds(PAD + SEGMENTS[c][0], SEGMENTS[c][1]), :],
            row_send.at[side, c], row_recv.at[side, c], (harm, tx + 1 - 2 * side, ty),
        )

    def col_copy(side):
        return remote(
            S.at[:, 4:8, pl.ds(PAD if side else PAD + COLS - 8, 8), :],
            S.at[:, 4:8, pl.ds(PAD + COLS if side else PAD - 8, 8), :],
            col_send.at[side], col_recv.at[side], (harm, tx, ty + 1 - 2 * side),
        )

    def corner_copy(side, vertical):
        at = PAD + COLS if side else PAD - 8
        return remote(
            S.at[:, 4:8, pl.ds(at, 8), :],
            S.at[:, pl.ds(8 * vertical, 4), pl.ds(at, 8), :],
            corner_send.at[side, vertical], corner_recv.at[side, vertical],
            (harm, tx + 1 - 2 * vertical, ty),
        )

    def to_side(side):
        return tx < TX - 1 if side == 0 else tx > 0

    def from_side(side):
        return tx > 0 if side == 0 else tx < TX - 1

    def to_col(side):
        return ty < TY - 1 if side == 0 else ty > 0

    def from_col(side):
        return ty > 0 if side == 0 else ty < TY - 1

    for side in (0, 1):
        @pl.when(to_col(side))
        def _():
            col_copy(side).start()
    def start_rows(c):
        for side in (0, 1):
            @pl.when(to_side(side))
            def _():
                row_copy(side, c).start()

    for c in range(4):
        start_rows(c)

    def early_copy(dy, dx):
        slot = 3 * (dy + 1) + dx + 1
        return remote(
            early.at[1, 1], early.at[1 - dy, 1 - dx], early_send.at[slot], early_recv.at[8 - slot],
            (harm, tx + dy, ty + dx),
        )

    def late_copy(dy):
        return remote(
            late.at[1], late.at[1 - dy], late_send.at[1 + dy], late_recv.at[1 - dy], (harm, tx + dy, ty),
        )

    def late_arrival(dy):
        return remote(
            late.at[1], late.at[1 + dy], late_send.at[1 + dy], late_recv.at[1 + dy], (harm, tx + dy, ty),
        )

    for dy, dx in AROUND:
        @pl.when(inside(dy, dx))
        def _():
            early_copy(dy, dx).start()

    lane = lax.broadcasted_iota(jnp.int32, (1, OWN), 1)
    gain = diffraction_gain / (harm * OWN + lane + 1).astype(F32)

    def row_inside(row):
        at = tx * ROWS + row - 4
        return jnp.where(jnp.logical_and(at >= 0, at < TX * ROWS), 1.0, 0.0).astype(F32)

    def stencil(c):
        base, width = SEGMENTS[c]
        for k, source, target in ((1, S, VA), (2, VA, VB), (3, VB, VA), (4, VA, M)):
            low, count = (12, width) if k == 4 else (8, width + 8)
            shift = base + 4 if k == 1 else 0
            at = ty * COLS + base + low + 4 - PAD + lax.broadcasted_iota(jnp.int32, (count, OWN), 0)
            valid = jnp.logical_and(at >= 0, at < TY * COLS)
            g = jnp.where(valid, gain * (1.0 / (5 - k)), 0.0)

            def one_row(row, carry):
                gr = g * row_inside(row)
                laps = []
                for p in range(2):
                    center = source[p, row, pl.ds(shift + low, count), :]
                    laps.append(
                        source[p, row + 1, pl.ds(shift + low, count), :]
                        + source[p, row - 1, pl.ds(shift + low, count), :]
                        + source[p, row, pl.ds(shift + low + 1, count), :]
                        + source[p, row, pl.ds(shift + low - 1, count), :]
                        - 4.0 * center
                    )
                real = S[0, row, pl.ds(base + 4 + low, count), :] - gr * laps[1]
                imag = S[1, row, pl.ds(base + 4 + low, count), :] + gr * laps[0]
                if k == 4:
                    target[0, row - 4, pl.ds(base, count), :] = real
                    target[1, row - 4, pl.ds(base, count), :] = imag
                else:
                    target[0, row, pl.ds(low, count), :] = real
                    target[1, row, pl.ds(low, count), :] = imag
                return carry

            lax.fori_loop(k, 12 - k, one_row, 0)

    def one_copy(c, row):
        return remote(
            M.at[:, row, pl.ds(*SEGMENTS[c]), :],
            R.at[harm, :, pl.ds(*SEGMENTS[c]), :],
            one_send.at[c, row], one_recv.at[c, harm], owner(row),
        )

    def one_arrival(c, at, width, j):
        return remote(
            M.at[:, 0, pl.ds(at, width), :],
            R.at[j, :, pl.ds(at, width), :],
            one_send.at[c, 0], one_recv.at[c, j], (j, tx, far_ty),
        )

    def two_copy(c, j):
        return remote(
            Y.at[j, :, pl.ds(c * PART, PART), :],
            field.at[own_row, :, pl.ds(c * PART, PART), :],
            two_send.at[c, j], two_recv.at[c, own_row], (j, tx, far_ty),
        )

    def two_arrival(c, row):
        return remote(
            Y.at[0, :, pl.ds(c * PART, PART), :],
            field.at[row, :, pl.ds(c * PART, PART), :],
            two_send.at[c, 0], two_recv.at[c, row], owner(row),
        )

    def wait_rows(c):
        for side in (0, 1):
            @pl.when(from_side(side))
            def _():
                row_copy(side, c).wait_recv()

    def forward(side):
        @pl.when(from_col(side))
        def _():
            col_copy(side).wait_recv()
            for vertical in (0, 1):
                @pl.when(to_side(vertical))
                def _():
                    corner_copy(side, vertical).start()

    def wait_corners(side):
        @pl.when(from_col(side))
        def _():
            for vertical in (0, 1):
                @pl.when(from_side(vertical))
                def _():
                    corner_copy(side, vertical).wait_recv()

    def build_tables():
        for copy in loads:
            copy.wait()

        def by_time(i, carry):
            rows = pl.ds(pl.multiple_of(i * 16, 16), 16)
            fc = factors_fine[0, rows, :]
            fs = factors_fine[1, rows, :]
            for a in range(8):
                ac = factors_coarse[0, a]
                as_ = factors_coarse[1, a]
                for table, value in ((synth_c, ac * fc - as_ * fs), (synth_s, as_ * fc + ac * fs)):
                    high, low = split(value)
                    table[0, rows, a * 128:(a + 1) * 128] = high
                    table[1, rows, a * 128:(a + 1) * 128] = low
            return carry

        lax.fori_loop(0, HARMONICS // 16, by_time, 0)

        def by_harmonic(a, carry):
            rows = pl.ds(pl.multiple_of(a * 16, 16), 16)
            ac = factors_far[0, pl.ds(a, 1), :]
            as_ = factors_far[1, pl.ds(a, 1), :]
            nc = factors_near[0]
            ns = factors_near[1]
            for table, value in ((anal_c, ac * nc - as_ * ns), (anal_s, as_ * nc + ac * ns)):
                high, low = split(value)
                table[0, rows, :] = high
                table[1, rows, :] = low
            return carry

        lax.fori_loop(0, HALF // 16, by_harmonic, 0)

    forward(0)
    for c in range(4, 7):
        start_rows(c)
    forward(1)
    for c in range(7, CHUNKS):
        start_rows(c)
    arrived = 0
    for c in ORDER:
        while arrived < min(c + 2, CHUNKS):
            wait_rows(arrived)
            arrived += 1
        if c == 0:
            wait_corners(0)
        if c == CHUNKS - 1:
            wait_corners(1)
        stencil(c)
        for row in range(ROWS):
            one_copy(c, row).start()
    build_tables()

    numbers = (lax.broadcasted_iota(jnp.int32, (1, HARMONICS), 1) + 1).astype(F32)
    scale = 2.0 * math.sqrt(HARMONICS) / CYCLE_READINGS / HARMONICS
    real_factor = numbers * (nonlinear_gain / HARMONICS * 4.0 * scale)
    imag_factor = numbers * (nonlinear_gain / HARMONICS * 2.0 * scale)

    def nonlinear(c, carry):
        @pl.when(c == 0)
        def _():
            for k in range(4):
                for j in range(4):
                    one_arrival(k, 8 * k, 8, j).wait_recv()

        @pl.when(c > 0)
        def _():
            for k in range(2):
                for j in range(4):
                    one_arrival(2 + 2 * c + k, pl.multiple_of(c * PART + 16 * k, 16), 16, j).wait_recv()

        cols = pl.ds(pl.multiple_of(c * PART, PART), PART)
        real = jnp.concatenate([R[j, 0, cols, :] for j in range(4)], axis=1)
        imag = jnp.concatenate([R[j, 1, cols, :] for j in range(4)], axis=1)
        even = product(real, synth_c[0], synth_c[1])
        odd = product(imag, synth_s[0], synth_s[1])
        cosine = product(even * even + odd * odd, anal_c[0], anal_c[1])
        sine = product(even * odd, anal_s[0], anal_s[1])
        real = real - real_factor * sine
        imag = imag + imag_factor * cosine
        weighted = numbers * (real * real + imag * imag)
        W[cols, :] = weighted[:, 0:128] + weighted[:, 128:256] + weighted[:, 256:384] + weighted[:, 384:512]
        for j in range(4):
            Y[j, 0, cols, :] = real[:, 128 * j:128 * (j + 1)]
            Y[j, 1, cols, :] = imag[:, 128 * j:128 * (j + 1)]

        @pl.when(c < EARLY_PARTS)
        def _():
            for j in range(4):
                two_copy(c, j).start()

        return carry

    lax.fori_loop(0, PARTS, nonlinear, 0)

    heat_out[...] = lax.dot_general(
        jnp.ones((8, OWN), F32), W[...], (((1,), (1,)), ((), ())),
        precision=lax.Precision.HIGHEST, preferred_element_type=F32,
    )[0:1]

    def heat_copy(dx, j):
        return remote(
            heat_out, heat_rows.at[1 - dx, own_row], heat_send.at[1 + dx, j], heat_recv.at[1 - dx, own_row],
            (j, tx, (ty + dx + 4) % TY),
        )

    def heat_arrival(dx, row):
        return remote(
            heat_out, heat_rows.at[1 + dx, row], heat_send.at[1, 0], heat_recv.at[1 + dx, row],
            (row, tx, far_ty),
        )

    def reached(dx):
        return far_ty > 0 if dx < 0 else far_ty < TY - 1

    for j in range(4):
        heat_copy(0, j).start()
    for dx in (-1, 1):
        @pl.when(reached(dx))
        def _():
            for j in range(4):
                heat_copy(dx, j).start()
    for c in range(EARLY_PARTS, PARTS):
        for j in range(4):
            two_copy(c, j).start()
    for row in range(ROWS):
        heat_arrival(0, row).wait_recv()
    for dx in (-1, 1):
        @pl.when(inside(0, dx))
        def _():
            for row in range(ROWS):
                heat_arrival(dx, row).wait_recv()
    for dx in range(3):
        for row in range(ROWS):
            late[1, dx, row:row + 1, :] = heat_rows[dx, row]
    for dy in (-1, 1):
        @pl.when(inside(dy, 0))
        def _():
            late_copy(dy).start()
    for dy, dx in AROUND:
        @pl.when(inside(dy, dx))
        def _():
            early_copy(-dy, -dx).wait_recv()
    for dy in (-1, 1):
        @pl.when(inside(dy, 0))
        def _():
            late_arrival(dy).wait_recv()
    for dy in range(3):
        for dx in range(3):
            rows = slice(4 * dy, 4 * dy + 4)
            cols = slice(128 * dx, 128 * dx + 128)
            for k in range(4):
                wide[k, rows, cols] = early[dy, dx, k]
            wide[4, rows, cols] = late[dy, dx]
    for k in range(5):
        wide[k, 12:16, :] = jnp.zeros((4, 3 * COLS), F32)
    temperature = wide[0]
    wide_conduct = wide[1]
    wide_perfuse = wide[2]
    wide_deposit = wide[3] * wide[4] / float(HARMONICS * HARMONICS)
    for _ in range(4):
        lap = (
            pltpu.roll(temperature, 15, 0) + pltpu.roll(temperature, 1, 0)
            + pltpu.roll(temperature, 3 * COLS - 1, 1) + pltpu.roll(temperature, 1, 1)
            - 4.0 * temperature
        )
        temperature = temperature + wide_conduct * lap - wide_perfuse * temperature + wide_deposit
    wide[0] = temperature
    later[...] = wide[0, 4:8, COLS:2 * COLS]

    for side in (0, 1):
        @pl.when(to_col(side))
        def _():
            col_copy(side).wait_send()
        for c in range(CHUNKS):
            @pl.when(to_side(side))
            def _():
                row_copy(side, c).wait_send()

        @pl.when(from_col(side))
        def _():
            for vertical in (0, 1):
                @pl.when(to_side(vertical))
                def _():
                    corner_copy(side, vertical).wait_send()
    for dy, dx in AROUND:
        @pl.when(inside(dy, dx))
        def _():
            early_copy(dy, dx).wait_send()
    for dy in (-1, 1):
        @pl.when(inside(dy, 0))
        def _():
            late_copy(dy).wait_send()
    for j in range(4):
        heat_copy(0, j).wait_send()
    for dx in (-1, 1):
        @pl.when(reached(dx))
        def _():
            for j in range(4):
                heat_copy(dx, j).wait_send()
    for c in range(CHUNKS):
        for j in range(4):
            one_copy(c, j).wait_send()
    for c in range(PARTS):
        for j in range(4):
            two_copy(c, j).wait_send()
            two_arrival(c, j).wait_recv()


def solution(mesh):
    factors = table_factors()

    def body(wave, lens, label, prior, attenuation, drain, diffusivity):
        vmem = pl.BlockSpec(memory_space=pltpu.VMEM)
        anywhere = pl.BlockSpec(memory_space=pl.ANY)
        def in_hbm(x):
            return pltpu.with_memory_space_constraint(x, pltpu.HBM)

        hbm = pl.BlockSpec(memory_space=pltpu.HBM)
        dma = pltpu.SemaphoreType.DMA
        field, later = pl.pallas_call(
            kernel,
            out_shape=(
                jax.ShapeDtypeStruct((ROWS, 2, COLS, OWN), F32),
                jax.ShapeDtypeStruct((ROWS, COLS), F32),
            ),
            in_specs=[hbm] * 15,
            out_specs=(anywhere, vmem),
            scratch_shapes=[
                pltpu.VMEM((ROWS, COLS), jnp.int32), pltpu.VMEM((ROWS, COLS), jnp.int32), pltpu.VMEM((ROWS, COLS), F32),
                pltpu.SMEM((8,), F32), pltpu.SMEM((8,), F32), pltpu.SMEM((8,), F32),
                pltpu.VMEM((2, ROWS, OWN, COLS), F32),
                pltpu.VMEM((2, 12, COLS + 2 * PAD, OWN), F32),
                pltpu.VMEM((2, 12, WIDEST + 2 * PAD, OWN), F32),
                pltpu.VMEM((2, 12, WIDEST + 2 * PAD, OWN), F32),
                pltpu.VMEM((2, ROWS, COLS, OWN), F32),
                pltpu.VMEM((4, 2, COLS, OWN), F32),
                pltpu.VMEM((4, 2, COLS, OWN), F32),
                pltpu.VMEM((COLS, OWN), F32),
                pltpu.VMEM((2, HARMONICS, HALF), BF16),
                pltpu.VMEM((2, HARMONICS, HALF), BF16),
                pltpu.VMEM((2, HALF, HARMONICS), BF16),
                pltpu.VMEM((2, HALF, HARMONICS), BF16),
                pltpu.VMEM((2, HARMONICS, 128), F32),
                pltpu.VMEM((2, 8, 16, 128), F32),
                pltpu.VMEM((2, 64, HARMONICS), F32),
                pltpu.VMEM((2, 16, HARMONICS), F32),
                pltpu.VMEM((3, 3, 4, ROWS, COLS), F32),
                pltpu.VMEM((3, 3, ROWS, COLS), F32),
                pltpu.VMEM((3, ROWS, 1, COLS), F32),
                pltpu.VMEM((1, COLS), F32),
                pltpu.VMEM((5, 16, 3 * COLS), F32),
                dma((6,)), dma((2, ROWS)), dma((8,)), dma((2, CHUNKS)), dma((2, CHUNKS)), dma((2,)), dma((2,)), dma((2, 2)), dma((2, 2)),
                dma((9,)), dma((9,)), dma((3,)), dma((3,)),
                dma((CHUNKS, 4)), dma((CHUNKS, 4)), dma((PARTS, 4)), dma((PARTS, 4)), dma((3, 4)), dma((3, 4)),
            ],
            compiler_params=pltpu.CompilerParams(
                collective_id=0, has_side_effects=True, vmem_limit_bytes=48 << 20
            ),
            name="march",
        )(*[in_hbm(a) for a in (wave, lens, label, prior, attenuation, drain, diffusivity)], *[in_hbm(jnp.asarray(f)) for f in factors])
        return jnp.transpose(field, (1, 3, 0, 2)), later

    in_specs = (P(None, "harm", "tx", "ty"), P("tx", "ty"), P("tx", "ty"), P("tx", "ty"), P(), P(), P())
    out_specs = (P(None, "harm", "tx", "ty"), P("tx", "ty"))
    return jax.shard_map(body, mesh=mesh, in_specs=in_specs, out_specs=out_specs, check_vma=False)
```
